8 devices in a mesh: rep: 2 (over y, z), dp: 4 (over x, core).
Axes of the slice: x: 2, y: 2, z: 1, core: 2. Of those that a mesh axis runs over, the one named last changes fastest.
Arguments:
- x: bfloat16 [8, 2048, 896], P(('rep', 'dp')), parts along dimension 0
- dy: bfloat16 [8, 2048, 896], P(('rep', 'dp')), parts along dimension 0
- w_gate: bfloat16 [2, 896, 2304], replicated
- w_up: bfloat16 [2, 896, 2304], replicated
- w_down: bfloat16 [2, 2304, 896], replicated
- m_w_gate: float32 [2, 896, 2304], P(None, 'dp')
- m_w_up: float32 [2, 896, 2304], P(None, 'dp')
- m_w_down: float32 [2, 2304, 896], P(None, 'dp')
- v_w_gate: float32 [2, 896, 2304], P(None, 'dp')
- v_w_up: float32 [2, 896, 2304], P(None, 'dp')
- v_w_down: float32 [2, 2304, 896], P(None, 'dp')
Outputs:
- output 1: bfloat16 [4, 896, 2304], P('rep'), parts along dimension 0
- output 2: bfloat16 [4, 896, 2304], P('rep'), parts along dimension 0
- output 3: bfloat16 [4, 2304, 896], P('rep'), parts along dimension 0
- output 4: float32 [4, 896, 2304], P('rep', 'dp'), parts along dimension 0
- output 5: float32 [4, 896, 2304], P('rep', 'dp'), parts along dimension 0
- output 6: float32 [4, 2304, 896], P('rep', 'dp'), parts along dimension 0
- output 7: float32 [4, 896, 2304], P('rep', 'dp'), parts along dimension 0
- output 8: float32 [4, 896, 2304], P('rep', 'dp'), parts along dimension 0
- output 9: float32 [4, 2304, 896], P('rep', 'dp'), parts along dimension 0
There are 2 independent parts. The reference program is written for one: setup_inputs(seed, part) draws one part's arguments, and reference() takes and returns one part's arrays. A program takes and returns all parts, laid end to end along the dimension named above; an argument that names none is the same for every part.
All inputs are finite; a program needn't handle non-finite values.
Results may differ from the reference program's by a relative error of at most 0.02.
Values are sent between devices in bfloat16 or wider.
A program may use at most 2 GiB of HBM per device.

```python
import jax
import jax.numpy as jnp
from jax import lax

SEQUENCES = 4
TOKENS = 2048
D = 896
FF = 2304
LAYERS = 2
NAMES = ("w_gate", "w_up", "w_down")
SHAPES = {"w_gate": (LAYERS, D, FF), "w_up": (LAYERS, D, FF), "w_down": (LAYERS, FF, D)}


def bump(key, n, height):
    away = (jnp.arange(n, dtype=jnp.int32) - jax.random.randint(key, (), 0, n, jnp.int32)) % n
    return jnp.where(away < n // 8, height, 1.0)


def together(key, own, strength):
    shared = jax.random.normal(key, own.shape[1:], jnp.float32)
    return (own + strength * shared) * lax.rsqrt(1 + strength * strength)


def setup_inputs(seed: int = 0, part: int = 0) -> dict:
    kx, kdy, ka, kb, kz, kf, kh, kl, *keys = jax.random.split(jax.random.key(seed), 8 + 3 * len(NAMES))
    kx, kdy, ka, kb = (jax.random.fold_in(k, part) for k in (kx, kdy, ka, kb))
    kw, km, kv = (keys[i::3] for i in range(3))
    shape = (SEQUENCES, TOKENS, D)
    much_x, much_dy = jax.random.uniform(kz, (2,), jnp.float32, 0.0, 1.0)
    loud = 2.0 ** jax.random.uniform(jax.random.fold_in(kz, 1), (), jnp.float32, -1.0, 2.0)
    layers = 2.0 ** jax.random.uniform(kl, (LAYERS, 1, 1), jnp.float32, -1.0, 1.0)
    x = together(ka, jax.random.normal(kx, shape, jnp.float32), much_x) * bump(kf, D, 4.0)
    dy = together(kb, jax.random.normal(kdy, shape, jnp.float32), much_dy)
    drawn = {"x": x.astype(jnp.bfloat16), "dy": (loud * dy * (SEQUENCES * TOKENS) ** -0.5).astype(jnp.bfloat16)}
    for key, name in zip(kw, NAMES, strict=True):
        w = jax.random.normal(key, SHAPES[name], jnp.float32) * SHAPES[name][1] ** -0.5
        drawn[name] = (w * {"w_gate": 1.0, "w_up": bump(kh, FF, 4.0), "w_down": layers}[name]).astype(jnp.bfloat16)
    for key, name in zip(km, NAMES, strict=True):
        drawn[f"m_{name}"] = 0.1 * jax.random.normal(key, SHAPES[name], jnp.float32)
    for key, name in zip(kv, NAMES, strict=True):
        drawn[f"v_{name}"] = jax.random.uniform(key, SHAPES[name], jnp.float32, 0.005, 0.015)
    return drawn


def matmul(a, w):
    return jnp.dot(a, w, preferred_element_type=jnp.float32).astype(jnp.bfloat16)


def normed(h):
    wide = h.astype(jnp.float32)
    scale = lax.rsqrt(jnp.mean(wide**2, -1, keepdims=True) + 1e-6)
    return (wide * scale).astype(jnp.bfloat16)


def layer(h, w):
    a = normed(h)
    gate = jnp.dot(a, w["w_gate"], preferred_element_type=jnp.float32)
    up = jnp.dot(a, w["w_up"], preferred_element_type=jnp.float32)
    return h + matmul((jax.nn.silu(gate) * up).astype(jnp.bfloat16), w["w_down"])


def adamw(w, m, v, g):
    m = 0.9 * m + 0.1 * g
    v = 0.95 * v + 0.05 * g * g
    step = m * lax.rsqrt(v + 1e-8) + 0.1 * w
    return (w - 0.02 * step).astype(jnp.bfloat16), m, v


def stack(weights, h):
    return lax.scan(lambda h, w: (layer(h, w), None), h, weights)[0]


def reference(x, dy, w_gate, w_up, w_down, m_w_gate, m_w_up, m_w_down, v_w_gate, v_w_up, v_w_down):
    weights = dict(zip(NAMES, (w_gate, w_up, w_down), strict=True))

    def take(so_far, sequence):
        h, by_y = sequence
        _, back = jax.vjp(lambda w: stack(w, h), weights)
        return jax.tree.map(lambda total, term: total + term.astype(jnp.float32), so_far, back(by_y)[0]), None

    none_yet = {name: jnp.zeros(w.shape, jnp.float32) for name, w in weights.items()}
    by_weights, _ = lax.scan(take, none_yet, (x, dy))
    gradients = [by_weights[name].astype(jnp.bfloat16).astype(jnp.float32) for name in NAMES]
    new = [
        adamw(w.astype(jnp.float32), m, v, g)
        for w, m, v, g in zip((w_gate, w_up, w_down), (m_w_gate, m_w_up, m_w_down), (v_w_gate, v_w_up, v_w_down), gradients, strict=True)
    ]
    return tuple(one[which] for which in range(3) for one in new)
```

```python
import functools

import jax
import jax.numpy as jnp
from jax import lax
from jax.experimental import pallas as pl
from jax.experimental.pallas import tpu as pltpu
from jax.sharding import PartitionSpec as P


F32, BF16 = jnp.float32, jnp.bfloat16
VMEM_LIMIT = 60 * 2**20


def dot(a, b, contract=((1,), (0,))):
    return lax.dot_general(a, b, (contract, ((), ())), preferred_element_type=F32)


def normed(h):
    scale = lax.rsqrt(jnp.mean(h * h, -1, keepdims=True) + 1e-6)
    return (h * scale).astype(BF16), scale


def call(body, at, args, specs, outs, out_specs, grid, scratch=(), aliases=None, flops=0, moved=0, after=()):
    n = len(args)
    args, specs = list(args) + list(after), list(specs) + [ANY] * len(after)
    return pl.pallas_call(
        lambda at, *refs: body(at, *refs[:n], *refs[n + len(after) :]),
        grid_spec=pltpu.PrefetchScalarGridSpec(
            num_scalar_prefetch=1, grid=grid, in_specs=specs, out_specs=out_specs, scratch_shapes=list(scratch)
        ),
        out_shape=outs,
        input_output_aliases={k + 1: v for k, v in (aliases or {}).items()},
        compiler_params=pltpu.CompilerParams(
            dimension_semantics=("arbitrary",) * len(grid), vmem_limit_bytes=VMEM_LIMIT
        ),
        cost_estimate=pl.CostEstimate(flops=int(flops), bytes_accessed=int(moved), transcendentals=0),
    )(at, *args)


def spec(shape, index, once=False):
    if once:
        return pl.BlockSpec(shape, index, pipeline_mode=pl.Buffered(1))
    return pl.BlockSpec(shape, index)


ANY = pl.BlockSpec(memory_space=pl.ANY)


def silu(gate):
    t = 0.5 * jnp.tanh(0.5 * gate)
    s = 0.5 + t
    p = gate * s
    return p, s + p * (0.5 - t)


def store_transposed(at, a, to):
    turned = a.T
    rows = turned.shape[0] // 4
    for owner in range(4):
        place = 2 * jnp.where(at[1] == owner % 2, 1, 0) + jnp.where(at[0] == owner // 2, 1, 0)
        to[pl.ds(pl.multiple_of(place * rows, rows), rows), :] = turned[owner * rows : (owner + 1) * rows]


def forward_body(at, x_ref, wg_ref, wu_ref, wd_ref, a0t_ref, p_ref, q_ref, act_ref, h_ref, a1_ref, a1t_ref):
    x = x_ref[0].astype(F32)
    a, _ = normed(x)
    store_transposed(at, a, a0t_ref)
    ff = wg_ref.shape[1]
    piece = ff // 3
    for lo in range(0, ff, piece):
        cut = slice(lo, lo + piece)
        gate, up = dot(a, wg_ref[:, cut]), dot(a, wu_ref[:, cut])
        p, slope = silu(gate)
        p_ref[:, cut] = p
        q_ref[:, cut] = up * slope
        act_ref[:, cut] = (p * up).astype(BF16)
    out = dot(act_ref[...], wd_ref[...]).astype(BF16)
    h = (x + out.astype(F32)).astype(BF16)
    h_ref[...] = h
    a1, _ = normed(h.astype(F32))
    a1_ref[...] = a1
    store_transposed(at, a1, a1t_ref)


def top_body(steps, at, a_ref, dy_ref, wg_ref, wu_ref, wd_ref, dgu_ref, theirs_ref, mine_ref, acc):
    step = pl.program_id(0)
    a, dy = a_ref[...], dy_ref[0]
    half = wg_ref.shape[1]
    gate, up = dot(a, wg_ref[...]), dot(a, wu_ref[...])
    d_act = dot(dy, wd_ref[...], ((1,), (1,))).astype(BF16).astype(F32)
    p, slope = silu(gate)
    act = (p * up).astype(BF16)
    dgu_ref[:, :half] = (d_act * (up * slope)).astype(BF16)
    dgu_ref[:, half:] = (d_act * p).astype(BF16)
    term = dot(act, dy, ((0,), (0,)))

    @pl.when(step == 0)
    def _():
        acc[...] = term

    @pl.when(step > 0)
    def _():
        acc[...] += term

    @pl.when(step == steps - 1)
    def _():
        rows = half // 2
        mine_ref[...] = acc[pl.ds(pl.multiple_of(at[1] * rows, rows), rows), :].astype(BF16)
        theirs_ref[...] = acc[pl.ds(pl.multiple_of((1 - at[1]) * rows, rows), rows), :].astype(BF16)


def wide_body(at, t_ref, d_ref, theirs_ref, other_ref, mine_ref):
    g = dot(t_ref[...], d_ref[...]).astype(BF16)
    rows = g.shape[0] // 4
    theirs_ref[0] = g[:rows]
    theirs_ref[1] = g[rows : 2 * rows]
    other_ref[...] = g[2 * rows : 3 * rows]
    mine_ref[...] = g[3 * rows :]


def back_body(at, da_ref, db_ref, wg_ref, wu_ref, h_ref, dy_ref, wd_ref, p_ref, q_ref, dg_ref, du_ref, d_out_ref):
    half = wg_ref.shape[1] // 2
    first = pl.ds(pl.multiple_of((1 - at[0]) * half, half), half)
    second = pl.ds(pl.multiple_of(at[0] * half, half), half)
    turn = ((1,), (1,))
    by_gate = dot(da_ref[:, :half], wg_ref[:, first], turn) + dot(db_ref[:, :half], wg_ref[:, second], turn)
    by_up = dot(da_ref[:, half:], wu_ref[:, first], turn) + dot(db_ref[:, half:], wu_ref[:, second], turn)
    d_a = by_gate.astype(BF16).astype(F32) + by_up.astype(BF16).astype(F32)
    h = h_ref[...].astype(F32)
    scale = lax.rsqrt(jnp.mean(h * h, -1, keepdims=True) + 1e-6)
    along = jnp.mean(d_a * h, -1, keepdims=True)
    d_h = (scale * d_a - h * (scale * scale * scale * along)).astype(BF16)
    d_out = (dy_ref[0].astype(F32) + d_h.astype(F32)).astype(BF16)
    d_out_ref[...] = d_out
    d_act = dot(d_out, wd_ref[...], turn).astype(BF16).astype(F32)
    dg_ref[...] = (d_act * q_ref[...]).astype(BF16)
    du_ref[...] = (d_act * p_ref[...]).astype(BF16)


def down_body(steps, at, act_ref, d_ref, theirs_ref, other_ref, mine_ref, acc):
    step = pl.program_id(0)
    term = dot(act_ref[...], d_ref[...], ((0,), (0,)))

    @pl.when(step == 0)
    def _():
        acc[...] = term

    @pl.when(step > 0)
    def _():
        acc[...] += term

    @pl.when(step == steps - 1)
    def _():
        rows = acc.shape[0] // 4

        def block(chip, core):
            return acc[pl.ds(pl.multiple_of((2 * chip + core) * rows, rows), rows), :].astype(BF16)

        theirs_ref[0] = block(1 - at[0], 1 - at[1])
        theirs_ref[1] = block(at[0], 1 - at[1])
        other_ref[...] = block(1 - at[0], at[1])
        mine_ref[...] = block(at[0], at[1])


def adamw(w, m, v, g):
    m = 0.9 * m + 0.1 * g
    v = 0.95 * v + 0.05 * g * g
    step = m * lax.rsqrt(v + 1e-8) + 0.1 * w
    return (w - 0.02 * step).astype(BF16), m, v


def adamw_body(parts, n_old, at, mine_ref, near_ref, far_ref, *refs):
    ins, outs = refs[: 3 * parts], refs[3 * parts + n_old :]
    g = mine_ref[...].astype(F32) + near_ref[...].astype(F32) + far_ref[...].astype(F32)
    g = g.astype(BF16).astype(F32)
    width = g.shape[1] // parts
    for k in range(parts):
        w_ref, m_ref, v_ref = ins[3 * k : 3 * k + 3]
        cut = slice(k * width, (k + 1) * width)
        w, m, v = adamw(w_ref[...].astype(F32), m_ref[...], v_ref[...], g[:, cut])
        outs[0][:, cut] = w
        outs[1 + 2 * k][...] = m
        outs[2 + 2 * k][...] = v


def place_body(parts, at, *refs):
    sources, outs = refs[:4], refs[-parts:]
    which = pl.program_id(0)
    for k in range(4):
        @pl.when(which == k)
        def _(k=k):
            width = sources[k].shape[1] // parts
            for j in range(parts):
                outs[j][...] = sources[k][:, j * width : (j + 1) * width]


def per_device(x, dy, wg, wu, wd, mg, mu, md, vg, vu, vd):
    _, tokens, d = x.shape
    _, _, ff = wg.shape
    half = ff // 2
    place = lax.axis_index("dp")
    chip, core = place // 2, place % 2
    at = jnp.stack([chip, core]).astype(jnp.int32)
    tile = 256
    steps = tokens // tile
    mm = 2 * tokens * d * ff

    def shape(*s, t=BF16):
        return jax.ShapeDtypeStruct(s, t)

    def over_x(value):
        return lax.ppermute(value, "dp", [(0, 2), (1, 3), (2, 0), (3, 1)])

    def over_core(value):
        return lax.ppermute(value, "dp", [(0, 1), (1, 0), (2, 3), (3, 2)])

    rows = lambda i, at: (i, 0)
    seq = spec((1, tile, d), lambda i, at: (0, i, 0))
    whole = lambda layer: (lambda i, at: (layer, 0, 0))

    a0t, p0, q0, act0, h1, a1, a1t = call(
        forward_body, at, (x, wg, wu, wd),
        [seq, spec((None, d, ff), whole(0), True), spec((None, d, ff), whole(0), True), spec((None, ff, d), whole(0), True)],
        [shape(d, tokens), shape(tokens, ff, t=F32), shape(tokens, ff, t=F32), shape(tokens, ff), shape(tokens, d), shape(tokens, d), shape(d, tokens)],
        [spec((d, tile), lambda i, at: (0, i)), spec((tile, ff), rows), spec((tile, ff), rows), spec((tile, ff), rows),
         spec((tile, d), rows), spec((tile, d), rows), spec((d, tile), lambda i, at: (0, i))],
        (steps,), flops=3 * mm, moved=70e6,
    )

    def top(which, after=()):
        col = lambda at: 1 - at[0] if which == 0 else at[0]
        return call(
            functools.partial(top_body, steps), at, (a1, dy, wg, wu, wd),
            [spec((tile, d), rows), seq, spec((None, d, half), lambda i, at: (1, 0, col(at)), True),
             spec((None, d, half), lambda i, at: (1, 0, col(at)), True), spec((None, half, d), lambda i, at: (1, col(at), 0), True)],
            [shape(tokens, ff), shape(half // 2, d), shape(half // 2, d)],
            [spec((tile, ff), rows)] + [spec((half // 2, d), lambda i, at: (0, 0))] * 2,
            (steps,), [pltpu.VMEM((half, d), F32)], flops=2 * mm, moved=25e6, after=after,
        )

    def wide(t, dgu, after=()):
        n = ff // 3
        r = d // 4
        return call(
            wide_body, at, (t, dgu),
            [spec((d, tokens), lambda i, at: (0, 0), True), spec((tokens, n), lambda i, at: (0, i))],
            [shape(2, r, ff), shape(r, ff), shape(r, ff)],
            [spec((2, r, n), lambda i, at: (0, 0, i)), spec((r, n), lambda i, at: (0, i)), spec((r, n), lambda i, at: (0, i))],
            (3,), flops=mm, moved=17e6, after=after,
        )

    def chip_sum(other, near):
        return (other.astype(F32) + near.astype(F32)).astype(BF16)

    def update(mine, near, far, layer, parts, cols, old, after=()):
        n_rows, n_cols = mine.shape
        width = n_cols // len(parts)
        tile_r = n_rows // 2 if n_rows == 224 else n_rows // 3
        n = n_rows // tile_r
        flat = spec((tile_r, n_cols), rows)
        specs = [flat, flat if near.ndim == 2 else spec((None, tile_r, n_cols), lambda i, at: (1, i, 0)), flat]
        args = [mine, near, far]
        outs, out_specs = [shape(n_rows, n_cols)], [flat]
        for w, m, v in parts:
            local = spec((None, tile_r, width), lambda i, at: (layer, i, cols(at)))
            specs += [spec((None, tile_r, width), lambda i, at: (layer, (2 * at[0] + at[1]) * n + i, cols(at))), local, local]
            args += [w, m, v]
            outs += [shape(*m.shape, t=F32)] * 2
            out_specs += [local, local]
        aliases = {}
        for k, o in enumerate(old):
            aliases[len(args)] = 1 + k
            args.append(o)
            specs.append(ANY)
        got = call(
            functools.partial(adamw_body, len(parts), len(old)), at, args, specs, outs, out_specs, (n,),
            aliases=aliases, flops=20e6, moved=20 * n_rows * n_cols, after=after,
        )
        return got[0], got[1:]

    def put(new, far, layer, shapes, cols, old, after=()):
        sources = new, over_core(new), far, over_core(far)
        n_rows, n_cols = new.shape
        width = n_cols // len(shapes)
        flat = spec((n_rows, n_cols), lambda i, at: (0, 0), True)

        def to(i, at):
            its_chip = jnp.where(i < 2, at[0], 1 - at[0])
            its_core = jnp.where(i % 2 == 0, at[1], 1 - at[1])
            return layer, 2 * its_chip + its_core, cols((its_chip, its_core))

        args = list(sources) + list(old)
        return call(
            functools.partial(place_body, len(shapes)), at, args, [flat] * 4 + [ANY] * len(old),
            [shape(*s) for s in shapes], [spec((None, n_rows, width), to)] * len(shapes), (4,),
            aliases={4 + k: k for k in range(len(old))}, flops=1e6, moved=16 * n_rows * n_cols, after=after,
        )

    none = lambda at: 0
    cols_a, cols_b = (lambda at: 1 - at[0]), (lambda at: at[0])
    gu = [(wg, mg, vg), (wu, mu, vu)]
    r = ff // 4

    dgu_a, theirs, other = top(0)
    s = chip_sum(other, over_core(theirs))
    far_d1 = over_x(s)
    theirs, other, mine_gua = wide(a1t, dgu_a, [s])
    near_gua = over_core(theirs)
    s = chip_sum(other, near_gua[0])
    far_gua = over_x(s)
    dgu_b, theirs, mine_d1 = top(1, [s])
    n_d1, old_d = update(mine_d1, over_core(theirs), far_d1, 1, [(wd, md, vd)], none, [])
    all_d1 = over_x(n_d1)
    theirs, other, mine_gub = wide(a1t, dgu_b, [n_d1])
    near_gub = over_core(theirs)
    s = chip_sum(other, near_gub[0])
    far_gub = over_x(s)
    n_gub, old_gu = update(mine_gub, near_gub, far_gua, 1, gu, cols_b, [], [s])
    all_gub = over_x(n_gub)

    dg0, du0, d_out = call(
        back_body, at, (dgu_a, dgu_b, wg, wu, h1, dy, wd, p0, q0),
        [spec((tile, ff), rows), spec((tile, ff), rows), spec((None, d, ff), whole(1), True), spec((None, d, ff), whole(1), True),
         spec((tile, d), rows), seq, spec((None, ff, d), whole(0), True), spec((tile, ff), rows), spec((tile, ff), rows)],
        [shape(tokens, ff), shape(tokens, ff), shape(tokens, d)],
        [spec((tile, ff), rows), spec((tile, ff), rows), spec((tile, d), rows)],
        (steps,), flops=3 * mm, moved=90e6, after=[n_gub],
    )
    n_gua, old_gu = update(mine_gua, near_gua, far_gub, 1, gu, cols_a, old_gu, [d_out])
    all_gua = over_x(n_gua)
    theirs, other, mine_d0 = call(
        functools.partial(down_body, steps), at, (act0, d_out),
        [spec((tile, ff), rows), spec((tile, d), rows)],
        [shape(2, r, d), shape(r, d), shape(r, d)],
        [spec((2, r, d), lambda i, at: (0, 0, 0), True), spec((r, d), lambda i, at: (0, 0), True), spec((r, d), lambda i, at: (0, 0), True)],
        (steps,), [pltpu.VMEM((ff, d), F32)], flops=mm, moved=17e6, after=[n_gua],
    )
    near_d0 = over_core(theirs)
    s = chip_sum(other, near_d0[0])
    far_d0 = over_x(s)
    theirs, other, mine_g0 = wide(a0t, dg0, [s])
    near_g0 = over_core(theirs)
    s = chip_sum(other, near_g0[0])
    far_g0 = over_x(s)
    theirs, other, mine_u0 = wide(a0t, du0, [s])
    near_u0 = over_core(theirs)
    s = chip_sum(other, near_u0[0])
    far_u0 = over_x(s)
    n_d0, new_d = update(mine_d0, near_d0, far_d0, 0, [(wd, md, vd)], none, old_d, [s])
    all_d0 = over_x(n_d0)
    out_d = put(n_d1, all_d1, 1, [wd.shape], none, [], [n_d0])
    out_gu = put(n_gub, all_gub, 1, [wg.shape, wu.shape], cols_b, [], out_d)
    n_g0, new_g = update(mine_g0, near_g0, far_g0, 0, gu[:1], none, old_gu[:2], out_gu[:1])
    all_g0 = over_x(n_g0)
    out_gu = put(n_gua, all_gua, 1, [wg.shape, wu.shape], cols_a, out_gu, [n_g0])
    n_u0, new_u = update(mine_u0, near_u0, far_u0, 0, gu[1:], none, old_gu[2:], out_gu[:1])
    all_u0 = over_x(n_u0)
    out_d = put(n_d0, all_d0, 0, [wd.shape], none, out_d, [n_u0])
    out_g = put(n_g0, all_g0, 0, [wg.shape], none, out_gu[:1], out_d)
    out_u = put(n_u0, all_u0, 0, [wu.shape], none, out_gu[1:], out_g)
    return out_g[0], out_u[0], out_d[0], new_g[0], new_u[0], new_d[0], new_g[1], new_u[1], new_d[1]


def solution(mesh):
    whole, part = P(None, None, None), P(None, "dp", None)
    seqs = P(("rep", "dp"), None, None)

    return jax.shard_map(
        per_device,
        mesh=mesh,
        in_specs=(seqs, seqs, whole, whole, whole) + (part,) * 6,
        out_specs=(P("rep", None, None),) * 3 + (P("rep", "dp", None),) * 6,
        check_vma=False,
    )
```

```python
import functools

import jax
import jax.numpy as jnp
from jax import lax
from jax.experimental import pallas as pl
from jax.experimental.pallas import tpu as pltpu
from jax.sharding import PartitionSpec as P


F32, BF16 = jnp.float32, jnp.bfloat16
MIB = 2**20


def dot(a, b, contract=((1,), (0,))):
    return lax.dot_general(a, b, (contract, ((), ())), preferred_element_type=F32)


def normed(h):
    scale = lax.rsqrt(jnp.mean(h * h, -1, keepdims=True) + 1e-6)
    return (h * scale).astype(BF16), scale


def call(body, at, args, specs, outs, out_specs, grid, scratch=(), aliases=None, flops=0, moved=0, after=(), vmem=60):
    n = len(args)
    args, specs = list(args) + list(after), list(specs) + [ANY] * len(after)
    return pl.pallas_call(
        lambda at, *refs: body(at, *refs[:n], *refs[n + len(after) :]),
        grid_spec=pltpu.PrefetchScalarGridSpec(
            num_scalar_prefetch=1, grid=grid, in_specs=specs, out_specs=out_specs, scratch_shapes=list(scratch)
        ),
        out_shape=outs,
        input_output_aliases={k + 1: v for k, v in (aliases or {}).items()},
        compiler_params=pltpu.CompilerParams(
            dimension_semantics=("arbitrary",) * len(grid), vmem_limit_bytes=vmem * MIB
        ),
        cost_estimate=pl.CostEstimate(flops=int(flops), bytes_accessed=int(moved), transcendentals=0),
    )(at, *args)


def call_with_partner(body, identity, args, specs, outs, out_specs, grid, scratch, flops, moved, after=(), vmem=60):
    n = len(args)
    args, specs = list(args) + list(after), list(specs) + [ANY] * len(after)
    return pl.pallas_call(
        lambda *refs: body(*refs[:n], *refs[n + len(after) :]),
        grid=grid,
        in_specs=specs,
        out_specs=out_specs,
        scratch_shapes=list(scratch),
        out_shape=outs,
        compiler_params=pltpu.CompilerParams(
            dimension_semantics=("arbitrary",) * len(grid), vmem_limit_bytes=vmem * MIB,
            collective_id=identity, has_side_effects=True,
        ),
        cost_estimate=pl.CostEstimate(flops=int(flops), bytes_accessed=int(moved), transcendentals=0),
    )(*args)


def place():
    at = lax.axis_index("dp")
    chip, core = at // 2, at % 2
    return chip, core, {"dp": 2 * chip + 1 - core}


def greet(partner):
    barrier = pltpu.get_barrier_semaphore()
    pl.semaphore_signal(barrier, inc=1, device_id=partner, device_id_type=pl.DeviceIdType.MESH)
    pl.semaphore_wait(barrier, 1)


def to_partner(source, target, send_sem, recv_sem, partner):
    return pltpu.make_async_remote_copy(
        source, target, send_sem, recv_sem, device_id=partner, device_id_type=pl.DeviceIdType.MESH
    )


def spec(shape, index, once=False):
    if once:
        return pl.BlockSpec(shape, index, pipeline_mode=pl.Buffered(1))
    return pl.BlockSpec(shape, index)


ANY = pl.BlockSpec(memory_space=pl.ANY)


def silu(gate):
    t = 0.5 * jnp.tanh(0.5 * gate)
    s = 0.5 + t
    p = gate * s
    return p, s + p * (0.5 - t)


def store_transposed(at, a, to):
    turned = a.T
    rows = turned.shape[0] // 4
    for owner in range(4):
        place = 2 * jnp.where(at[1] == owner % 2, 1, 0) + jnp.where(at[0] == owner // 2, 1, 0)
        to[pl.ds(pl.multiple_of(place * rows, rows), rows), :] = turned[owner * rows : (owner + 1) * rows]


def forward_body(at, x_ref, wg_ref, wu_ref, wd_ref, a0t_ref, p_ref, q_ref, act_ref, h_ref, a1_ref, a1t_ref):
    x = x_ref[0].astype(F32)
    a, _ = normed(x)
    store_transposed(at, a, a0t_ref)
    ff = wg_ref.shape[1]
    piece = ff // 3
    for lo in range(0, ff, piece):
        cut = slice(lo, lo + piece)
        gate, up = dot(a, wg_ref[:, cut]), dot(a, wu_ref[:, cut])
        p, slope = silu(gate)
        p_ref[:, cut] = p
        q_ref[:, cut] = up * slope
        act_ref[:, cut] = (p * up).astype(BF16)
    out = dot(act_ref[...], wd_ref[...]).astype(BF16)
    h = (x + out.astype(F32)).astype(BF16)
    h_ref[...] = h
    a1, _ = normed(h.astype(F32))
    a1_ref[...] = a1
    store_transposed(at, a1, a1t_ref)


def owned(half, core):
    own = half // 2
    extra = own % 128
    start = core * (own - extra)
    return pl.ds(pl.multiple_of(start, 128), own + extra), pl.ds(pl.multiple_of(core * extra, 16), own)


def top_body(
    which, steps, a_ref, dy_ref, wg_hbm, wu_hbm, wd_hbm, dy_hbm, dgu_ref, out_ref,
    w_s, wd_s, dy_s, act_s, send, keep, recv, sems, send_sem, recv_sem,
):
    step = pl.program_id(0)
    chip, core, partner = place()
    half = wd_s.shape[0]
    tile = a_ref.shape[0]
    first = (1 - chip if which == 0 else chip) * half
    cols = pl.ds(pl.multiple_of(first, 128), half)
    loads = [
        pltpu.make_async_copy(wg_hbm.at[1, :, cols], w_s.at[:, :half], sems.at[0]),
        pltpu.make_async_copy(wu_hbm.at[1, :, cols], w_s.at[:, half:], sems.at[1]),
        pltpu.make_async_copy(wd_hbm.at[1, cols, :], wd_s, sems.at[2]),
        pltpu.make_async_copy(dy_hbm.at[0], dy_s, sems.at[3]),
    ]

    @pl.when(step == 0)
    def _():
        for load in loads:
            load.start()
        greet(partner)
        for load in loads[:3]:
            load.wait()

    a, dy = a_ref[...], dy_ref[0]
    both = dot(a, w_s[...])
    gate, up = both[:, :half], both[:, half:]
    d_act = dot(dy, wd_s[...], ((1,), (1,))).astype(BF16).astype(F32)
    p, slope = silu(gate)
    act_s[pl.ds(pl.multiple_of(step * tile, tile), tile), :] = (p * up).astype(BF16)
    dgu_ref[:, :half] = (d_act * (up * slope)).astype(BF16)
    dgu_ref[:, half:] = (d_act * p).astype(BF16)

    @pl.when(step == steps - 1)
    def _():
        loads[3].wait()
        theirs, their_rows = owned(half, 1 - core)
        mine, my_rows = owned(half, core)
        send[...] = dot(act_s[:, theirs], dy_s[...], ((0,), (0,))).astype(BF16)
        copy = to_partner(send.at[their_rows], recv, send_sem, recv_sem, partner)
        copy.start()
        keep[...] = dot(act_s[:, mine], dy_s[...], ((0,), (0,))).astype(BF16)
        copy.wait()
        out_ref[...] = (keep[my_rows, :].astype(F32) + recv[...].astype(F32)).astype(out_ref.dtype)


def wide_body(steps, t_ref, d_ref, out_ref, part_ref, send, keep, recv, send_sem, recv_sem):
    step = pl.program_id(0)
    _, _, partner = place()
    rows, n = out_ref.shape[0], d_ref.shape[1]

    @pl.when(step == 0)
    def _():
        greet(partner)

    def copy(k):
        return to_partner(send.at[k], recv.at[k], send_sem.at[k], recv_sem.at[k], partner)

    def fold(k):
        copy(k).wait()
        cols = pl.ds(pl.multiple_of(k * n, 128), n)
        out_ref[:, cols] = (keep[k, :rows].astype(F32) + recv[k, :rows].astype(F32)).astype(BF16)
        part_ref[:, cols] = keep[k, rows:].astype(F32) + recv[k, rows:].astype(F32)

    g = dot(t_ref[...], d_ref[...]).astype(BF16)
    send[step] = g[: 2 * rows]
    keep[step] = g[2 * rows :]
    copy(step).start()

    @pl.when(step > 0)
    def _():
        fold(step - 1)

    @pl.when(step == steps - 1)
    def _():
        fold(step)


def down_body(act_ref, d_ref, out_ref, part_ref, send, keep, recv, send_sem, recv_sem):
    step = pl.program_id(0)
    chip, core, partner = place()
    half = act_ref.shape[1]
    theirs, their_rows = owned(half, 1 - core)
    mine, my_rows = owned(half, core)

    @pl.when(step == 0)
    def _():
        greet(partner)

    def copy(k):
        return to_partner(send.at[k, their_rows], recv.at[k], send_sem.at[k], recv_sem.at[k], partner)

    send[step] = dot(act_ref[:, theirs], d_ref[...], ((0,), (0,))).astype(BF16)
    copy(step).start()
    keep[step] = dot(act_ref[:, mine], d_ref[...], ((0,), (0,))).astype(BF16)

    @pl.when(step == 1)
    def _():
        for k in range(2):
            copy(k).wait()
        out_ref[...] = (keep[1 - chip, my_rows, :].astype(F32) + recv[1 - chip].astype(F32)).astype(BF16)
        part_ref[...] = keep[chip, my_rows, :].astype(F32) + recv[chip].astype(F32)


def back_body(at, da_ref, db_ref, wg_ref, wu_ref, h_ref, dy_ref, d_out_ref):
    half = wg_ref.shape[1] // 2
    first = pl.ds(pl.multiple_of((1 - at[0]) * half, half), half)
    second = pl.ds(pl.multiple_of(at[0] * half, half), half)
    turn = ((1,), (1,))
    by_gate = dot(wg_ref[:, first], da_ref[:, :half], turn) + dot(wg_ref[:, second], db_ref[:, :half], turn)
    by_up = dot(wu_ref[:, first], da_ref[:, half:], turn) + dot(wu_ref[:, second], db_ref[:, half:], turn)
    d_a = (by_gate.astype(BF16).astype(F32) + by_up.astype(BF16).astype(F32)).T
    h = h_ref[...].astype(F32)
    scale = lax.rsqrt(jnp.mean(h * h, -1, keepdims=True) + 1e-6)
    along = jnp.mean(d_a * h, -1, keepdims=True)
    d_h = (scale * d_a - h * (scale * scale * scale * along)).astype(BF16)
    d_out_ref[...] = (dy_ref[0].astype(F32) + d_h.astype(F32)).astype(BF16)


def bottom_body(steps, d_out_ref, t_ref, wd_ref, p_ref, q_ref, out_ref, part_ref, dgu, send, keep, recv, send_sem, recv_sem):
    step = pl.program_id(0)
    _, _, partner = place()
    rows, n = out_ref.shape[0], wd_ref.shape[0]

    @pl.when(step == 0)
    def _():
        greet(partner)

    def copy(k):
        return to_partner(send.at[k], recv.at[k], send_sem.at[k], recv_sem.at[k], partner)

    def fold(k):
        copy(k).wait()
        for p in range(2):
            cut = slice(p * n, (p + 1) * n)
            cols = pl.ds(pl.multiple_of((p * steps + k) * n, 128), n)
            out_ref[:, cols] = (keep[k, :rows, cut].astype(F32) + recv[k, :rows, cut].astype(F32)).astype(BF16)
            part_ref[:, cols] = keep[k, rows:, cut].astype(F32) + recv[k, rows:, cut].astype(F32)

    for lo in range(0, dgu.shape[0], 512):
        stretch = slice(lo, lo + 512)
        d_act = dot(d_out_ref[stretch, :], wd_ref[...], ((1,), (1,))).astype(BF16).astype(F32)
        dgu[stretch, :n] = (d_act * q_ref[stretch, :]).astype(BF16)
        dgu[stretch, n:] = (d_act * p_ref[stretch, :]).astype(BF16)
    g = dot(t_ref[...], dgu[...]).astype(BF16)
    send[step] = g[: 2 * rows]
    keep[step] = g[2 * rows :]
    copy(step).start()

    @pl.when(step > 0)
    def _():
        fold(step - 1)

    @pl.when(step == steps - 1)
    def _():
        fold(step)


def adamw(w, m, v, g):
    m = 0.9 * m + 0.1 * g
    v = 0.95 * v + 0.05 * g * g
    step = m * lax.rsqrt(v + 1e-8) + 0.1 * w
    return (w - 0.02 * step).astype(BF16), m, v


def adamw_body(parts, n_old, at, part_ref, far_ref, *refs):
    ins, outs = refs[: 3 * parts], refs[3 * parts + n_old :]
    width = part_ref.shape[1] // parts

    @pl.loop(0, part_ref.shape[0] // 16)
    def _(k):
        rows = pl.ds(pl.multiple_of(k * 16, 16), 16)
        for p in range(parts):
            cut = slice(p * width, (p + 1) * width)
            g = (part_ref[rows, cut] + far_ref[rows, cut].astype(F32)).astype(BF16).astype(F32)
            w_ref, m_ref, v_ref = ins[3 * p : 3 * p + 3]
            w, m, v = adamw(w_ref[rows, :].astype(F32), m_ref[rows, :], v_ref[rows, :], g)
            outs[0][rows, cut] = w
            outs[1 + 2 * p][rows, :] = m
            outs[2 + 2 * p][rows, :] = v


def put_body(parts, blocks, n_old, *refs):
    n = len(blocks)
    sources, outs = refs[:n], refs[n + n_old : n + n_old + parts]
    held, in_sems, out_sems = refs[n + n_old + parts :]
    chip, core, _ = place()
    reads = [pltpu.make_async_copy(sources[k], held.at[k], in_sems.at[k]) for k in range(n)]
    for read in reads:
        read.start()
    writes = []
    for k, (layer, far, other, first, half) in enumerate(blocks):
        reads[k].wait()
        rows, width = sources[k].shape
        width //= parts
        its_chip = 1 - chip if far else chip
        its_core = 1 - core if other else core
        own = outs[0].shape[1] // 4
        to_rows = pl.ds(pl.multiple_of((2 * its_chip + its_core) * own + first, 16), rows)
        if half is None:
            to_cols = slice(None)
        elif half is not True and half is not False:
            to_cols = pl.ds(half, width)
        else:
            to_cols = pl.ds(pl.multiple_of((its_chip if half else 1 - its_chip) * width, 128), width)
        for p in range(parts):
            write = pltpu.make_async_copy(
                held.at[k, :, pl.ds(p * width, width)], outs[p].at[layer, to_rows, to_cols], out_sems.at[k, p]
            )
            write.start()
            writes.append(write)
    for write in writes:
        write.wait()


def per_device(x, dy, wg, wu, wd, mg, mu, md, vg, vu, vd):
    _, tokens, d = x.shape
    _, _, ff = wg.shape
    half = ff // 2
    place = lax.axis_index("dp")
    chip, core = place // 2, place % 2
    at = jnp.stack([chip, core]).astype(jnp.int32)
    tile = 256
    steps = tokens // tile
    mm = 2 * tokens * d * ff

    def shape(*s, t=BF16):
        return jax.ShapeDtypeStruct(s, t)

    def over_x(value):
        return lax.ppermute(value, "dp", [(0, 2), (1, 3), (2, 0), (3, 1)])

    def over_core(value):
        return lax.ppermute(value, "dp", [(0, 1), (1, 0), (2, 3), (3, 2)])

    rows = lambda i, at: (i, 0)
    seq = spec((1, tile, d), lambda i, at: (0, i, 0))
    whole = lambda layer: (lambda i, at: (layer, 0, 0))

    a0t, p0, q0, act0, h1, a1, a1t = call(
        forward_body, at, (x, wg, wu, wd),
        [seq, spec((None, d, ff), whole(0), True), spec((None, d, ff), whole(0), True), spec((None, ff, d), whole(0), True)],
        [shape(d, tokens), shape(tokens, ff, t=F32), shape(tokens, ff, t=F32), shape(tokens, ff), shape(tokens, d), shape(tokens, d), shape(d, tokens)],
        [spec((d, tile), lambda i, at: (0, i)), spec((tile, ff), rows), spec((tile, ff), rows), spec((tile, ff), rows),
         spec((tile, d), rows), spec((tile, d), rows), spec((d, tile), lambda i, at: (0, i))],
        (steps,), flops=3 * mm, moved=70e6,
    )

    def buffers(slots, rows_sent, rows, n):
        lead = () if slots == 0 else (slots,)
        sem = pltpu.SemaphoreType.DMA if slots == 0 else pltpu.SemaphoreType.DMA((slots,))
        return [pltpu.VMEM((*lead, rows_sent, n), BF16), pltpu.VMEM((*lead, rows_sent, n), BF16), pltpu.VMEM((*lead, rows, n), BF16), sem, sem]

    def top(which, after=()):
        own = half // 2
        whole_out = spec((own, d), lambda i: (0, 0), True)
        send, keep, recv, sem, _ = buffers(0, own + own % 128, own, d)
        return call_with_partner(
            functools.partial(top_body, which, steps), which, (a1, dy, wg, wu, wd, dy),
            [spec((tile, d), lambda i: (i, 0)), spec((1, tile, d), lambda i: (0, i, 0)), ANY, ANY, ANY, ANY],
            [shape(tokens, ff), shape(own, d, t=F32 if which else BF16)],
            [spec((tile, ff), lambda i: (i, 0)), whole_out],
            (steps,),
            [pltpu.VMEM((d, ff), BF16), pltpu.VMEM((half, d), BF16), pltpu.VMEM((tokens, d), BF16), pltpu.VMEM((tokens, half), BF16),
             send, keep, recv, pltpu.SemaphoreType.DMA((4,)), sem, sem],
            2 * mm, 25e6, after,
        )

    def wide(identity, t, dgu, after=()):
        n = ff // 3
        r = d // 4
        full = spec((r, ff), lambda i: (0, 0), True)
        return call_with_partner(
            functools.partial(wide_body, 3), identity, (t, dgu),
            [spec((d, tokens), lambda i: (0, 0), True), spec((tokens, n), lambda i: (0, i))],
            [shape(r, ff), shape(r, ff, t=F32)], [full, full], (3,), buffers(3, 2 * r, 2 * r, n), mm, 17e6, after,
        )

    def update(part, far, layer, parts, cols, old, after=(), stretch=(0, 2)):
        n_rows, n_cols = part.shape
        width = n_cols // len(parts)
        first, n = stretch
        tiles = 2
        tile_r = n_rows // tiles
        flat = spec((tile_r, n_cols), lambda i, at: (first + i, 0))
        specs, args = [flat, flat], [part, far]
        outs, out_specs = [shape(n * tile_r, n_cols)], [spec((tile_r, n_cols), rows)]
        for w, m, v in parts:
            local = spec((None, tile_r, width), lambda i, at: (layer, first + i, cols(at)))
            specs += [spec((None, tile_r, width), lambda i, at: (layer, (2 * at[0] + at[1]) * tiles + first + i, cols(at))), local, local]
            args += [w, m, v]
            outs += [shape(*m.shape, t=F32)] * 2
            out_specs += [local, local]
        aliases = {}
        for k, o in enumerate(old):
            aliases[len(args)] = 1 + k
            args.append(o)
            specs.append(ANY)
        got = call(
            functools.partial(adamw_body, len(parts), len(old)), at, args, specs, outs, out_specs, (n,),
            aliases=aliases, flops=20e6, moved=20 * n_rows * n_cols, after=after,
        )
        return got[0], got[1:]

    def put(sources, blocks, shapes, old, after=()):
        n, parts = len(sources), len(shapes)
        args = list(sources) + list(old) + list(after)
        return pl.pallas_call(
            lambda *refs: put_body(parts, blocks, len(old) + len(after), *refs),
            in_specs=[ANY] * len(args),
            out_specs=[ANY] * parts,
            out_shape=[shape(*s) for s in shapes],
            scratch_shapes=[pltpu.VMEM((n, *sources[0].shape), BF16), pltpu.SemaphoreType.DMA((n,)), pltpu.SemaphoreType.DMA((n, parts))],
            input_output_aliases={n + k: k for k in range(len(old))},
            compiler_params=pltpu.CompilerParams(vmem_limit_bytes=60 * MIB),
            cost_estimate=pl.CostEstimate(flops=1000000, bytes_accessed=4000000 * n, transcendentals=0),
        )(*args)

    def put_all(new, far, layer, half, shapes, old, after=()):
        blocks = [(layer, f, o, 0, half) for f in (False, True) for o in (False, True)]
        return put([new, over_core(new), far, over_core(far)], blocks, shapes, old, after)

    none = lambda at: 0
    cols_a, cols_b = (lambda at: 1 - at[0]), (lambda at: at[0])
    gu = [(wg, mg, vg), (wu, mu, vu)]
    r = ff // 4

    dgu_a, s = top(0)
    far_d1 = over_x(s)
    s, part_gua = wide(2, a1t, dgu_a, [s])
    far_gua = over_x(s)
    dgu_b, part_d1 = top(1, [s])
    n_d1, old_d = update(part_d1, far_d1, 1, [(wd, md, vd)], none, [])
    all_d1 = over_x(n_d1)
    s, part_gub = wide(3, a1t, dgu_b, [n_d1])
    far_gub = over_x(s)
    n_gub, old_gu = update(part_gub, far_gua, 1, gu, cols_b, [])
    all_gub = over_x(n_gub)

    wide_tile = 512
    by_rows = lambda n: spec((wide_tile, n), rows)
    d_out = call(
        back_body, at, (dgu_a, dgu_b, wg, wu, h1, dy),
        [by_rows(ff), by_rows(ff), spec((None, d, ff), whole(1), True), spec((None, d, ff), whole(1), True),
         by_rows(d), spec((1, wide_tile, d), lambda i, at: (0, i, 0))],
        shape(tokens, d), by_rows(d), (tokens // wide_tile,), flops=2 * mm, moved=35e6, after=[n_gub],
    )

    def bottom(identity, first, steps, after):
        n, r = 256, d // 4
        cols = 2 * n * steps
        full = spec((r, cols), lambda i: (0, 0), True)
        to_cols = spec((tokens, n), lambda i: (0, first + i))
        return call_with_partner(
            functools.partial(bottom_body, steps), identity, (d_out, a0t, wd, p0, q0),
            [spec((tokens, d), lambda i: (0, 0), True), spec((d, tokens), lambda i: (0, 0), True),
             spec((None, n, d), lambda i: (0, first + i, 0)), to_cols, to_cols],
            [shape(r, cols), shape(r, cols, t=F32)], [full, full], (steps,),
            [pltpu.VMEM((tokens, 2 * n), BF16)] + buffers(steps, 2 * r, 2 * r, 2 * n),
            3 * mm * steps // 9, 50e6 * steps / 9, after,
        )

    n_gua, old_gu = update(part_gua, far_gub, 1, gu, cols_a, old_gu, [d_out])
    all_gua = over_x(n_gua)
    full = spec((r, d), lambda i: (0, 0), True)
    s, part_d0 = call_with_partner(
        down_body, 4, (act0, d_out), [spec((tokens, half), lambda i: (0, i)), spec((tokens, d), lambda i: (0, 0), True)],
        [shape(r, d), shape(r, d, t=F32)], [full, full], (2,), buffers(2, r + r % 128, r, d), mm, 17e6, [n_gua],
    )
    far_d0 = over_x(s)
    s, part_0 = bottom(5, 0, 6, [s])
    far_0 = over_x(s)
    s, part_1 = bottom(6, 6, 3, [s])
    far_1 = over_x(s)
    n_d0, new_d = update(part_d0, far_d0, 0, [(wd, md, vd)], none, old_d, [s])
    all_d0 = over_x(n_d0)
    both = [wg.shape, wu.shape]
    out_d = put_all(n_d1, all_d1, 1, None, [wd.shape], [], [n_d0])
    out_gu = put_all(n_gub, all_gub, 1, True, both, [], out_d)
    n_0, old_gu = update(part_0, far_0, 0, gu, none, old_gu, out_gu[:1])
    all_0 = over_x(n_0)
    out_gu = put_all(n_gua, all_gua, 1, False, both, out_gu, [n_0])
    third = lambda at: 2
    n_top, old_gu = update(part_1, far_1, 0, gu, third, old_gu, out_gu[:1], (0, 1))
    far_top = over_x(n_top)
    n_low, (mg, vg, mu, vu) = update(part_1, far_1, 0, gu, third, old_gu, [n_top], (1, 1))
    far_low = over_x(n_low)
    out_d = put_all(n_d0, all_d0, 0, None, [wd.shape], out_d, [n_low])
    first = n_top.shape[0]
    start = part_0.shape[1] // 2
    blocks = [(0, f, o, low, start) for f in (False, True) for low in (0, first) for o in (False, True)]
    out_gu = put([n_top, over_core(n_top), n_low, over_core(n_low)], blocks[:4], both, out_gu, out_d)
    out_gu = put_all(n_0, all_0, 0, 0, both, out_gu)
    out_gu = put([far_top, over_core(far_top)], blocks[4:6], both, out_gu)
    out_gu = put([far_low, over_core(far_low)], blocks[6:], both, out_gu)
    return out_gu[0], out_gu[1], out_d[0], mg, mu, new_d[0], vg, vu, new_d[1]


def solution(mesh):
    whole, part = P(None, None, None), P(None, "dp", None)
    seqs = P(("rep", "dp"), None, None)

    return jax.shard_map(
        per_device,
        mesh=mesh,
        in_specs=(seqs, seqs, whole, whole, whole) + (part,) * 6,
        out_specs=(P("rep", None, None),) * 3 + (P("rep", "dp", None),) * 6,
        check_vma=False,
    )
```

```python
import functools

import jax
import jax.numpy as jnp
from jax import lax
from jax.experimental import pallas as pl
from jax.experimental.pallas import tpu as pltpu
from jax.sharding import PartitionSpec as P


F32, BF16 = jnp.float32, jnp.bfloat16
MIB = 2**20


def dot(a, b, contract=((1,), (0,))):
    return lax.dot_general(a, b, (contract, ((), ())), preferred_element_type=F32)


def normed(h):
    scale = lax.rsqrt(jnp.mean(h * h, -1, keepdims=True) + 1e-6)
    return (h * scale).astype(BF16), scale


def call(body, at, args, specs, outs, out_specs, grid, scratch=(), aliases=None, flops=0, moved=0, after=(), vmem=60):
    n = len(args)
    args, specs = list(args) + list(after), list(specs) + [ANY] * len(after)
    return pl.pallas_call(
        lambda at, *refs: body(at, *refs[:n], *refs[n + len(after) :]),
        grid_spec=pltpu.PrefetchScalarGridSpec(
            num_scalar_prefetch=1, grid=grid, in_specs=specs, out_specs=out_specs, scratch_shapes=list(scratch)
        ),
        out_shape=outs,
        input_output_aliases={k + 1: v for k, v in (aliases or {}).items()},
        compiler_params=pltpu.CompilerParams(
            dimension_semantics=("arbitrary",) * len(grid), vmem_limit_bytes=vmem * MIB
        ),
        cost_estimate=pl.CostEstimate(flops=int(flops), bytes_accessed=int(moved), transcendentals=0),
    )(at, *args)


def call_with_partner(body, identity, args, specs, outs, out_specs, grid, scratch, flops, moved, after=(), vmem=60):
    n = len(args)
    args, specs = list(args) + list(after), list(specs) + [ANY] * len(after)
    return pl.pallas_call(
        lambda *refs: body(*refs[:n], *refs[n + len(after) :]),
        grid=grid,
        in_specs=specs,
        out_specs=out_specs,
        scratch_shapes=list(scratch),
        out_shape=outs,
        compiler_params=pltpu.CompilerParams(
            dimension_semantics=("arbitrary",) * len(grid), vmem_limit_bytes=vmem * MIB,
            collective_id=identity, has_side_effects=True,
        ),
        cost_estimate=pl.CostEstimate(flops=int(flops), bytes_accessed=int(moved), transcendentals=0),
    )(*args)


def place():
    at = lax.axis_index("dp")
    chip, core = at // 2, at % 2
    return chip, core, {"dp": 2 * chip + 1 - core}


def greet(partner):
    barrier = pltpu.get_barrier_semaphore()
    pl.semaphore_signal(barrier, inc=1, device_id=partner, device_id_type=pl.DeviceIdType.MESH)
    pl.semaphore_wait(barrier, 1)


def to_partner(source, target, send_sem, recv_sem, partner):
    return pltpu.make_async_remote_copy(
        source, target, send_sem, recv_sem, device_id=partner, device_id_type=pl.DeviceIdType.MESH
    )


def spec(shape, index, once=False):
    if once:
        return pl.BlockSpec(shape, index, pipeline_mode=pl.Buffered(1))
    return pl.BlockSpec(shape, index)


ANY = pl.BlockSpec(memory_space=pl.ANY)


def silu(gate):
    t = 0.5 * jnp.tanh(0.5 * gate)
    s = 0.5 + t
    p = gate * s
    return p, s + p * (0.5 - t)


def store_transposed(at, a, to):
    turned = a.T
    rows = turned.shape[0] // 4
    for owner in range(4):
        place = 2 * jnp.where(at[1] == owner % 2, 1, 0) + jnp.where(at[0] == owner // 2, 1, 0)
        to[pl.ds(pl.multiple_of(place * rows, rows), rows), :] = turned[owner * rows : (owner + 1) * rows]


def forward_body(
    ff_steps, at, x_ref, wg_ref, wu_ref, wd_hbm, a0t_ref, p_ref, q_ref, act_ref, h_ref, a1_ref, a1t_ref, a_s, act_s, wd_s, sem
):
    step = pl.program_id(0)
    tokens, n, tile, chunk = a_s.shape[0], wg_ref.shape[1], h_ref.shape[0], 256
    load = pltpu.make_async_copy(wd_hbm.at[0], wd_s, sem)

    def hidden(fresh, los):
        cols = slice(0, n) if fresh else pl.ds(pl.multiple_of(step * n, n), n)
        for lo in los:
            r = pl.ds(lo, chunk)
            if fresh:
                a, _ = normed(x_ref[0, r].astype(F32))
                a_s[r] = a
            else:
                a = a_s[r]
            gate, up = dot(a, wg_ref[...]), dot(a, wu_ref[...])
            p, slope = silu(gate)
            p_ref[r] = p
            q_ref[r] = up * slope
            act = (p * up).astype(BF16)
            act_ref[r] = act
            act_s[r, cols] = act

    @pl.when(step == 0)
    def _():
        load.start()
        hidden(True, range(0, tokens, chunk))

    @pl.when((step > 0) & (step < ff_steps))
    def _():
        hidden(False, range(0, tokens, chunk))

    @pl.when(step == ff_steps)
    def _():
        load.wait()

    @pl.when(step >= ff_steps)
    def _():
        base = (step - ff_steps) * tile
        for lo in range(0, tile, chunk):
            r = pl.ds(pl.multiple_of(base + lo, chunk), chunk)
            to = slice(lo, lo + chunk)
            out = dot(act_s[r], wd_s[...]).astype(BF16)
            h = (x_ref[0, r].astype(F32) + out.astype(F32)).astype(BF16)
            h_ref[to] = h
            a1_ref[to] = normed(h.astype(F32))[0]
        store_transposed(at, a1_ref[...], a1t_ref)
        store_transposed(at, a_s[pl.ds(pl.multiple_of(base, tile), tile)], a0t_ref)


def owned(half, core):
    own = half // 2
    extra = own % 128
    start = core * (own - extra)
    return pl.ds(pl.multiple_of(start, 128), own + extra), pl.ds(pl.multiple_of(core * extra, 16), own)


def top_body(
    which, steps, a_ref, dy_ref, wg_hbm, wu_hbm, wd_hbm, dy_hbm, dgu_ref, out_ref,
    w_s, wd_s, dy_s, act_s, both, recv, sems, send_sem, recv_sem,
):
    step = pl.program_id(0)
    chip, core, partner = place()
    half = wd_s.shape[0]
    tile = a_ref.shape[0]
    first = (1 - chip if which == 0 else chip) * half
    cols = pl.ds(pl.multiple_of(first, 128), half)
    loads = [
        pltpu.make_async_copy(wg_hbm.at[1, :, cols], w_s.at[:, :half], sems.at[0]),
        pltpu.make_async_copy(wu_hbm.at[1, :, cols], w_s.at[:, half:], sems.at[1]),
        pltpu.make_async_copy(wd_hbm.at[1, cols, :], wd_s, sems.at[2]),
        pltpu.make_async_copy(dy_hbm.at[0], dy_s, sems.at[3]),
    ]

    @pl.when(step == 0)
    def _():
        for load in loads[:3]:
            load.start()
        greet(partner)
        for load in loads[:3]:
            load.wait()
        loads[3].start()

    a, dy = a_ref[...], dy_ref[0]
    hidden = dot(a, w_s[...])
    gate, up = hidden[:, :half], hidden[:, half:]
    d_act = dot(dy, wd_s[...], ((1,), (1,))).astype(BF16).astype(F32)
    p, slope = silu(gate)
    act_s[pl.ds(pl.multiple_of(step * tile, tile), tile), :] = (p * up).astype(BF16)
    dgu_ref[:, :half] = (d_act * (up * slope)).astype(BF16)
    dgu_ref[:, half:] = (d_act * p).astype(BF16)

    @pl.when(step == steps - 1)
    def _():
        loads[3].wait()
        _, their_rows = owned(half, 1 - core)
        _, my_rows = owned(half, core)
        copy = to_partner(both.at[0, their_rows], recv, send_sem, recv_sem, partner)

        @pl.loop(0, 2)
        def _(k):
            cols, _ = owned(half, jnp.where(k == 0, 1 - core, core))
            both[k] = dot(act_s[:, cols], dy_s[...], ((0,), (0,))).astype(BF16)

            @pl.when(k == 0)
            def _():
                copy.start()

        copy.wait()
        out_ref[...] = (both[1, my_rows, :].astype(F32) + recv[...].astype(F32)).astype(out_ref.dtype)


def wide_body(steps, t_ref, d_ref, out_ref, part_ref, send, keep, recv, send_sem, recv_sem):
    step = pl.program_id(0)
    _, _, partner = place()
    rows, n = out_ref.shape[0], d_ref.shape[1]

    @pl.when(step == 0)
    def _():
        greet(partner)

    def copy(k):
        return to_partner(send.at[k], recv.at[k], send_sem.at[k], recv_sem.at[k], partner)

    def fold(k):
        copy(k).wait()
        cols = pl.ds(pl.multiple_of(k * n, 128), n)
        out_ref[:, cols] = (keep[k, :rows].astype(F32) + recv[k, :rows].astype(F32)).astype(BF16)
        part_ref[:, cols] = keep[k, rows:].astype(F32) + recv[k, rows:].astype(F32)

    g = dot(t_ref[...], d_ref[...]).astype(BF16)
    send[step] = g[: 2 * rows]
    keep[step] = g[2 * rows :]
    copy(step).start()

    @pl.when(step > 0)
    def _():
        fold(step - 1)

    @pl.when(step == steps - 1)
    def _():
        fold(step)


def down_body(act_ref, d_ref, out_ref, part_ref, both, recv, send_sem, recv_sem):
    step = pl.program_id(0)
    chip, core, partner = place()
    half = act_ref.shape[1]
    _, their_rows = owned(half, 1 - core)
    _, my_rows = owned(half, core)

    @pl.when(step == 0)
    def _():
        greet(partner)

    def copy(k):
        return to_partner(both.at[0, k, their_rows], recv.at[k], send_sem.at[k], recv_sem.at[k], partner)

    @pl.loop(0, 2)
    def _(k):
        cols, _ = owned(half, jnp.where(k == 0, 1 - core, core))
        both[k, step] = dot(act_ref[:, cols], d_ref[...], ((0,), (0,))).astype(BF16)

        @pl.when(k == 0)
        def _():
            copy(step).start()

    @pl.when(step == 1)
    def _():
        for k in range(2):
            copy(k).wait()
        out_ref[...] = (both[1, 1 - chip, my_rows, :].astype(F32) + recv[1 - chip].astype(F32)).astype(BF16)
        part_ref[...] = both[1, chip, my_rows, :].astype(F32) + recv[chip].astype(F32)


def back_body(at, da_ref, db_ref, wg_hbm, wu_hbm, h_ref, dy_ref, d_out_ref, w_s, sems):
    step = pl.program_id(0)
    half = da_ref.shape[1] // 2
    loads = []
    for k, w in enumerate((wg_hbm, wu_hbm)):
        for which, chip in enumerate((1 - at[0], at[0])):
            cols = pl.ds(pl.multiple_of(chip * half, 128), half)
            loads.append(pltpu.make_async_copy(w.at[1, :, cols], w_s.at[k, :, which * half : (which + 1) * half], sems.at[k, which]))

    @pl.when(step == 0)
    def _():
        for load in loads:
            load.start()
        for load in loads:
            load.wait()

    chunk = 256
    for lo in range(0, h_ref.shape[0], chunk):
        r = slice(lo, lo + chunk)
        terms = []
        for k in range(2):
            cut = slice(k * half, (k + 1) * half)
            d = jnp.concatenate([da_ref[r, cut], db_ref[r, cut]], axis=1)
            terms.append(dot(w_s[k], d, ((1,), (1,))).astype(BF16).astype(F32))
        d_a = (terms[0] + terms[1]).T
        h = h_ref[r].astype(F32)
        scale = lax.rsqrt(jnp.mean(h * h, -1, keepdims=True) + 1e-6)
        along = jnp.mean(d_a * h, -1, keepdims=True)
        d_h = (scale * d_a - h * (scale * scale * scale * along)).astype(BF16)
        d_out_ref[r] = (dy_ref[0, r].astype(F32) + d_h.astype(F32)).astype(BF16)


def bottom_body(steps, d_out_ref, t_ref, wd_ref, p_ref, q_ref, out_ref, part_ref, dgu, send, keep, recv, send_sem, recv_sem):
    step = pl.program_id(0)
    _, _, partner = place()
    rows, n = out_ref.shape[0], wd_ref.shape[0]

    @pl.when(step == 0)
    def _():
        greet(partner)

    def copy(k):
        return to_partner(send.at[k], recv.at[k], send_sem.at[k], recv_sem.at[k], partner)

    def fold(k):
        copy(k).wait()
        for p in range(2):
            cut = slice(p * n, (p + 1) * n)
            cols = pl.ds(pl.multiple_of((p * steps + k) * n, 128), n)
            out_ref[:, cols] = (keep[k, :rows, cut].astype(F32) + recv[k, :rows, cut].astype(F32)).astype(BF16)
            part_ref[:, cols] = keep[k, rows:, cut].astype(F32) + recv[k, rows:, cut].astype(F32)

    for lo in range(0, dgu.shape[0], 512):
        stretch = slice(lo, lo + 512)
        d_act = dot(d_out_ref[stretch, :], wd_ref[...], ((1,), (1,))).astype(BF16).astype(F32)
        dgu[stretch, :n] = (d_act * q_ref[stretch, :]).astype(BF16)
        dgu[stretch, n:] = (d_act * p_ref[stretch, :]).astype(BF16)
    g = dot(t_ref[...], dgu[...]).astype(BF16)
    send[step] = g[: 2 * rows]
    keep[step] = g[2 * rows :]
    copy(step).start()

    @pl.when(step > 0)
    def _():
        fold(step - 1)

    @pl.when(step == steps - 1)
    def _():
        fold(step)


def adamw(w, m, v, g):
    m = 0.9 * m + 0.1 * g
    v = 0.95 * v + 0.05 * g * g
    step = m * lax.rsqrt(v + 1e-8) + 0.1 * w
    return (w - 0.02 * step).astype(BF16), m, v


def adamw_body(parts, n_old, at, part_ref, far_ref, *refs):
    ins, outs = refs[: 3 * parts], refs[3 * parts + n_old :]
    width = part_ref.shape[1] // parts

    @pl.loop(0, part_ref.shape[0] // 16)
    def _(k):
        rows = pl.ds(pl.multiple_of(k * 16, 16), 16)
        for p in range(parts):
            cut = slice(p * width, (p + 1) * width)
            g = (part_ref[rows, cut] + far_ref[rows, cut].astype(F32)).astype(BF16).astype(F32)
            w_ref, m_ref, v_ref = ins[3 * p : 3 * p + 3]
            w, m, v = adamw(w_ref[rows, :].astype(F32), m_ref[rows, :], v_ref[rows, :], g)
            outs[0][rows, cut] = w
            outs[1 + 2 * p][rows, :] = m
            outs[2 + 2 * p][rows, :] = v


def put_body(parts, blocks, n_old, *refs):
    n = len(blocks)
    sources, outs = refs[:n], refs[n + n_old : n + n_old + parts]
    held, in_sems, out_sems = refs[n + n_old + parts :]
    chip, core, _ = place()
    reads = [pltpu.make_async_copy(sources[k], held.at[k], in_sems.at[k]) for k in range(n)]
    for read in reads:
        read.start()
    writes = []
    for k, (layer, far, other, first, half) in enumerate(blocks):
        reads[k].wait()
        rows, width = sources[k].shape
        width //= parts
        its_chip = 1 - chip if far else chip
        its_core = 1 - core if other else core
        own = outs[0].shape[1] // 4
        to_rows = pl.ds(pl.multiple_of((2 * its_chip + its_core) * own + first, 16), rows)
        if half is None:
            to_cols = slice(None)
        elif half is not True and half is not False:
            to_cols = pl.ds(half, width)
        else:
            to_cols = pl.ds(pl.multiple_of((its_chip if half else 1 - its_chip) * width, 128), width)
        for p in range(parts):
            write = pltpu.make_async_copy(
                held.at[k, :, pl.ds(p * width, width)], outs[p].at[layer, to_rows, to_cols], out_sems.at[k, p]
            )
            write.start()
            writes.append(write)
    for write in writes:
        write.wait()


def per_device(x, dy, wg, wu, wd, mg, mu, md, vg, vu, vd):
    _, tokens, d = x.shape
    _, _, ff = wg.shape
    half = ff // 2
    place = lax.axis_index("dp")
    chip, core = place // 2, place % 2
    at = jnp.stack([chip, core]).astype(jnp.int32)
    tile = 256
    steps = tokens // tile
    mm = 2 * tokens * d * ff

    def shape(*s, t=BF16):
        return jax.ShapeDtypeStruct(s, t)

    def over_x(value):
        return lax.ppermute(value, "dp", [(0, 2), (1, 3), (2, 0), (3, 1)])

    def over_core(value):
        return lax.ppermute(value, "dp", [(0, 1), (1, 0), (2, 3), (3, 2)])

    rows = lambda i, at: (i, 0)
    seq = spec((1, tile, d), lambda i, at: (0, i, 0))

    n, by = 256, 512
    ff_steps = ff // n
    ff_tile = lambda i: jnp.minimum(i, ff_steps - 1)
    token_tile = lambda i: jnp.maximum(i - ff_steps, 0)
    w_tile = spec((None, d, n), lambda i, at: (0, 0, ff_tile(i)))
    by_ff = spec((tokens, n), lambda i, at: (0, ff_tile(i)))
    by_token = spec((by, d), lambda i, at: (token_tile(i), 0))
    turned = spec((d, by), lambda i, at: (0, token_tile(i)))
    a0t, p0, q0, act0, h1, a1, a1t = call(
        functools.partial(forward_body, ff_steps), at, (x, wg, wu, wd),
        [spec((1, tokens, d), lambda i, at: (0, 0, 0), True), w_tile, w_tile, ANY],
        [shape(d, tokens), shape(tokens, ff, t=F32), shape(tokens, ff, t=F32), shape(tokens, ff), shape(tokens, d), shape(tokens, d), shape(d, tokens)],
        [turned, by_ff, by_ff, by_ff, by_token, by_token, turned], (ff_steps + tokens // by,),
        [pltpu.VMEM((tokens, d), BF16), pltpu.VMEM((tokens, ff), BF16), pltpu.VMEM((ff, d), BF16), pltpu.SemaphoreType.DMA],
        flops=3 * mm, moved=70e6,
    )

    def buffers(slots, rows_sent, rows, n):
        sem = pltpu.SemaphoreType.DMA((slots,))
        return [pltpu.VMEM((slots, rows_sent, n), BF16), pltpu.VMEM((slots, rows_sent, n), BF16), pltpu.VMEM((slots, rows, n), BF16), sem, sem]

    def top(which, after=()):
        own = half // 2
        whole_out = spec((own, d), lambda i: (0, 0), True)
        sem = pltpu.SemaphoreType.DMA
        return call_with_partner(
            functools.partial(top_body, which, steps), which, (a1, dy, wg, wu, wd, dy),
            [spec((tile, d), lambda i: (i, 0)), spec((1, tile, d), lambda i: (0, i, 0)), ANY, ANY, ANY, ANY],
            [shape(tokens, ff), shape(own, d, t=F32 if which else BF16)],
            [spec((tile, ff), lambda i: (i, 0)), whole_out],
            (steps,),
            [pltpu.VMEM((d, ff), BF16), pltpu.VMEM((half, d), BF16), pltpu.VMEM((tokens, d), BF16), pltpu.VMEM((tokens, half), BF16),
             pltpu.VMEM((2, own + own % 128, d), BF16), pltpu.VMEM((own, d), BF16), sem((4,)), sem, sem],
            2 * mm, 25e6, after,
        )

    def wide(identity, t, dgu, after=()):
        n = ff // 3
        r = d // 4
        full = spec((r, ff), lambda i: (0, 0), True)
        return call_with_partner(
            functools.partial(wide_body, 3), identity, (t, dgu),
            [spec((d, tokens), lambda i: (0, 0), True), spec((tokens, n), lambda i: (0, i))],
            [shape(r, ff), shape(r, ff, t=F32)], [full, full], (3,), buffers(3, 2 * r, 2 * r, n), mm, 17e6, after,
        )

    def update(part, far, layer, parts, cols, old, after=(), stretch=(0, 2)):
        n_rows, n_cols = part.shape
        width = n_cols // len(parts)
        first, n = stretch
        tiles = 2
        tile_r = n_rows // tiles
        flat = spec((tile_r, n_cols), lambda i, at: (first + i, 0))
        specs, args = [flat, flat], [part, far]
        outs, out_specs = [shape(n * tile_r, n_cols)], [spec((tile_r, n_cols), rows)]
        for w, m, v in parts:
            local = spec((None, tile_r, width), lambda i, at: (layer, first + i, cols(at)))
            specs += [spec((None, tile_r, width), lambda i, at: (layer, (2 * at[0] + at[1]) * tiles + first + i, cols(at))), local, local]
            args += [w, m, v]
            outs += [shape(*m.shape, t=F32)] * 2
            out_specs += [local, local]
        aliases = {}
        for k, o in enumerate(old):
            aliases[len(args)] = 1 + k
            args.append(o)
            specs.append(ANY)
        got = call(
            functools.partial(adamw_body, len(parts), len(old)), at, args, specs, outs, out_specs, (n,),
            aliases=aliases, flops=20e6, moved=20 * n_rows * n_cols, after=after,
        )
        return got[0], got[1:]

    def put(sources, blocks, shapes, old, after=()):
        n, parts = len(sources), len(shapes)
        args = list(sources) + list(old) + list(after)
        return pl.pallas_call(
            lambda *refs: put_body(parts, blocks, len(old) + len(after), *refs),
            in_specs=[ANY] * len(args),
            out_specs=[ANY] * parts,
            out_shape=[shape(*s) for s in shapes],
            scratch_shapes=[pltpu.VMEM((n, *sources[0].shape), BF16), pltpu.SemaphoreType.DMA((n,)), pltpu.SemaphoreType.DMA((n, parts))],
            input_output_aliases={n + k: k for k in range(len(old))},
            compiler_params=pltpu.CompilerParams(vmem_limit_bytes=60 * MIB),
            cost_estimate=pl.CostEstimate(flops=1000000, bytes_accessed=4000000 * n, transcendentals=0),
        )(*args)

    def put_all(new, far, layer, half, shapes, old, after=()):
        blocks = [(layer, f, o, 0, half) for f in (False, True) for o in (False, True)]
        return put([new, over_core(new), far, over_core(far)], blocks, shapes, old, after)

    none = lambda at: 0
    cols_a, cols_b = (lambda at: 1 - at[0]), (lambda at: at[0])
    gu = [(wg, mg, vg), (wu, mu, vu)]
    r = ff // 4

    dgu_a, s = top(0)
    far_d1 = over_x(s)
    s, part_gua = wide(2, a1t, dgu_a, [s])
    far_gua = over_x(s)
    dgu_b, part_d1 = top(1, [s])
    n_d1, old_d = update(part_d1, far_d1, 1, [(wd, md, vd)], none, [])
    all_d1 = over_x(n_d1)
    s, part_gub = wide(3, a1t, dgu_b, [n_d1])
    far_gub = over_x(s)
    n_gub, old_gu = update(part_gub, far_gua, 1, gu, cols_b, [])
    all_gub = over_x(n_gub)

    wide_tile = 512
    by_rows = lambda n: spec((wide_tile, n), rows)
    d_out = call(
        back_body, at, (dgu_a, dgu_b, wg, wu, h1, dy),
        [by_rows(ff), by_rows(ff), ANY, ANY, by_rows(d), spec((1, wide_tile, d), lambda i, at: (0, i, 0))],
        shape(tokens, d), by_rows(d), (tokens // wide_tile,), [pltpu.VMEM((2, d, ff), BF16), pltpu.SemaphoreType.DMA((2, 2))], flops=2 * mm, moved=35e6, after=[n_gub],
    )

    def bottom(identity, first, steps, after):
        n, r = 256, d // 4
        cols = 2 * n * steps
        full = spec((r, cols), lambda i: (0, 0), True)
        to_cols = spec((tokens, n), lambda i: (0, first + i))
        return call_with_partner(
            functools.partial(bottom_body, steps), identity, (d_out, a0t, wd, p0, q0),
            [spec((tokens, d), lambda i: (0, 0), True), spec((d, tokens), lambda i: (0, 0), True),
             spec((None, n, d), lambda i: (0, first + i, 0)), to_cols, to_cols],
            [shape(r, cols), shape(r, cols, t=F32)], [full, full], (steps,),
            [pltpu.VMEM((tokens, 2 * n), BF16)] + buffers(steps, 2 * r, 2 * r, 2 * n),
            3 * mm * steps // 9, 50e6 * steps / 9, after,
        )

    n_gua, old_gu = update(part_gua, far_gub, 1, gu, cols_a, old_gu, [d_out])
    all_gua = over_x(n_gua)
    full = spec((r, d), lambda i: (0, 0), True)
    s, part_d0 = call_with_partner(
        down_body, 4, (act0, d_out), [spec((tokens, half), lambda i: (0, i)), spec((tokens, d), lambda i: (0, 0), True)],
        [shape(r, d), shape(r, d, t=F32)], [full, full], (2,), [pltpu.VMEM((2, 2, r + r % 128, d), BF16), pltpu.VMEM((2, r, d), BF16)] + [pltpu.SemaphoreType.DMA((2,))] * 2, mm, 17e6, [n_gua],
    )
    far_d0 = over_x(s)
    s, part_0 = bottom(5, 0, 6, [s])
    far_0 = over_x(s)
    s, part_1 = bottom(6, 6, 3, [s])
    far_1 = over_x(s)
    n_d0, new_d = update(part_d0, far_d0, 0, [(wd, md, vd)], none, old_d, [s])
    all_d0 = over_x(n_d0)
    both = [wg.shape, wu.shape]
    out_d = put_all(n_d1, all_d1, 1, None, [wd.shape], [], [n_d0])
    out_gu = put_all(n_gub, all_gub, 1, True, both, [], out_d)
    n_0, old_gu = update(part_0, far_0, 0, gu, none, old_gu, out_gu[:1])
    all_0 = over_x(n_0)
    out_gu = put_all(n_gua, all_gua, 1, False, both, out_gu, [n_0])
    third = lambda at: 2
    n_top, old_gu = update(part_1, far_1, 0, gu, third, old_gu, out_gu[:1], (0, 1))
    far_top = over_x(n_top)
    n_low, (mg, vg, mu, vu) = update(part_1, far_1, 0, gu, third, old_gu, [n_top], (1, 1))
    far_low = over_x(n_low)
    out_d = put_all(n_d0, all_d0, 0, None, [wd.shape], out_d, [n_low])
    first = n_top.shape[0]
    start = part_0.shape[1] // 2
    blocks = [(0, f, o, low, start) for f in (False, True) for low in (0, first) for o in (False, True)]
    out_gu = put([n_top, over_core(n_top), n_low, over_core(n_low)], blocks[:4], both, out_gu, out_d)
    out_gu = put_all(n_0, all_0, 0, 0, both, out_gu)
    out_gu = put([far_top, over_core(far_top)], blocks[4:6], both, out_gu)
    out_gu = put([far_low, over_core(far_low)], blocks[6:], both, out_gu)
    return out_gu[0], out_gu[1], out_d[0], mg, mu, new_d[0], vg, vu, new_d[1]


def solution(mesh):
    whole, part = P(None, None, None), P(None, "dp", None)
    seqs = P(("rep", "dp"), None, None)

    return jax.shard_map(
        per_device,
        mesh=mesh,
        in_specs=(seqs, seqs, whole, whole, whole) + (part,) * 6,
        out_specs=(P("rep", None, None),) * 3 + (P("rep", "dp", None),) * 6,
        check_vma=False,
    )
```

```python
import functools

import jax
import jax.numpy as jnp
from jax import lax
from jax.experimental import pallas as pl
from jax.experimental.pallas import tpu as pltpu
from jax.sharding import PartitionSpec as P


F32, BF16 = jnp.float32, jnp.bfloat16
MIB = 2**20


def dot(a, b, contract=((1,), (0,))):
    return lax.dot_general(a, b, (contract, ((), ())), preferred_element_type=F32)


def normed(h):
    scale = lax.rsqrt(jnp.mean(h * h, -1, keepdims=True) + 1e-6)
    return (h * scale).astype(BF16), scale


def call(body, at, args, specs, outs, out_specs, grid, scratch=(), aliases=None, flops=0, moved=0, after=(), vmem=60):
    n = len(args)
    args, specs = list(args) + list(after), list(specs) + [ANY] * len(after)
    return pl.pallas_call(
        lambda at, *refs: body(at, *refs[:n], *refs[n + len(after) :]),
        grid_spec=pltpu.PrefetchScalarGridSpec(
            num_scalar_prefetch=1, grid=grid, in_specs=specs, out_specs=out_specs, scratch_shapes=list(scratch)
        ),
        out_shape=outs,
        input_output_aliases={k + 1: v for k, v in (aliases or {}).items()},
        compiler_params=pltpu.CompilerParams(
            dimension_semantics=("arbitrary",) * len(grid), vmem_limit_bytes=vmem * MIB
        ),
        cost_estimate=pl.CostEstimate(flops=int(flops), bytes_accessed=int(moved), transcendentals=0),
    )(at, *args)


def call_with_partner(body, identity, args, specs, outs, out_specs, grid, scratch, flops, moved, after=(), vmem=60):
    n = len(args)
    args, specs = list(args) + list(after), list(specs) + [ANY] * len(after)
    return pl.pallas_call(
        lambda *refs: body(*refs[:n], *refs[n + len(after) :]),
        grid=grid,
        in_specs=specs,
        out_specs=out_specs,
        scratch_shapes=list(scratch),
        out_shape=outs,
        compiler_params=pltpu.CompilerParams(
            dimension_semantics=("arbitrary",) * len(grid), vmem_limit_bytes=vmem * MIB,
            collective_id=identity, has_side_effects=True,
        ),
        cost_estimate=pl.CostEstimate(flops=int(flops), bytes_accessed=int(moved), transcendentals=0),
    )(*args)


def place():
    at = lax.axis_index("dp")
    chip, core = at // 2, at % 2
    return chip, core, {"dp": 2 * chip + 1 - core}


def greet(partner):
    barrier = pltpu.get_barrier_semaphore()
    pl.semaphore_signal(barrier, inc=1, device_id=partner, device_id_type=pl.DeviceIdType.MESH)
    pl.semaphore_wait(barrier, 1)


def to_partner(source, target, send_sem, recv_sem, partner):
    return pltpu.make_async_remote_copy(
        source, target, send_sem, recv_sem, device_id=partner, device_id_type=pl.DeviceIdType.MESH
    )


def spec(shape, index, once=False):
    if once:
        return pl.BlockSpec(shape, index, pipeline_mode=pl.Buffered(1))
    return pl.BlockSpec(shape, index)


ANY = pl.BlockSpec(memory_space=pl.ANY)
TURNED, TALL = ((1,), (1,)), ((0,), (0,))


def CORNER(*_):
    return 0, 0


def silu(gate):
    t = 0.5 * jnp.tanh(0.5 * gate)
    s = 0.5 + t
    p = gate * s
    return p, s + p * (0.5 - t)


def store_transposed(at, a, to):
    turned = a.T
    rows = turned.shape[0] // 4
    for owner in range(4):
        place = 2 * jnp.where(at[1] == owner % 2, 1, 0) + jnp.where(at[0] == owner // 2, 1, 0)
        to[pl.ds(pl.multiple_of(place * rows, rows), rows), :] = turned[owner * rows : (owner + 1) * rows]


def forward_body(
    ff_steps, at, x_ref, wg_ref, wu_ref, wd_hbm, a0t_ref, p_ref, q_ref, act_ref, h_ref, a1_ref, a1t_ref, a_s, act_s, wd_s, sem
):
    step = pl.program_id(0)
    tokens, n, tile, chunk = a_s.shape[0], wg_ref.shape[1], h_ref.shape[0], 256
    load = pltpu.make_async_copy(wd_hbm.at[0], wd_s, sem)

    def hidden(fresh, los):
        cols = slice(0, n) if fresh else pl.ds(pl.multiple_of(step * n, n), n)
        for lo in los:
            r = pl.ds(lo, chunk)
            if fresh:
                a, _ = normed(x_ref[0, r].astype(F32))
                a_s[r] = a
            else:
                a = a_s[r]
            gate, up = dot(a, wg_ref[...]), dot(a, wu_ref[...])
            p, slope = silu(gate)
            p_ref[r] = p
            q_ref[r] = up * slope
            act = (p * up).astype(BF16)
            act_ref[r] = act
            act_s[r, cols] = act

    @pl.when(step == 0)
    def _():
        load.start()
        hidden(True, range(0, tokens, chunk))

    @pl.when((step > 0) & (step < ff_steps))
    def _():
        hidden(False, range(0, tokens, chunk))

    @pl.when(step == ff_steps)
    def _():
        load.wait()

    @pl.when(step >= ff_steps)
    def _():
        base = (step - ff_steps) * tile
        for lo in range(0, tile, chunk):
            r = pl.ds(pl.multiple_of(base + lo, chunk), chunk)
            to = slice(lo, lo + chunk)
            out = dot(act_s[r], wd_s[...]).astype(BF16)
            h = (x_ref[0, r].astype(F32) + out.astype(F32)).astype(BF16)
            h_ref[to] = h
            a1_ref[to] = normed(h.astype(F32))[0]
        store_transposed(at, a1_ref[...], a1t_ref)
        store_transposed(at, a_s[pl.ds(pl.multiple_of(base, tile), tile)], a0t_ref)


def owned(half, core):
    own = half // 2
    extra = own % 128
    start = core * (own - extra)
    return pl.ds(pl.multiple_of(start, 128), own + extra), pl.ds(pl.multiple_of(core * extra, 16), own)


def middle_body(
    steps, a_ref, dy_ref, wg_hbm, wu_hbm, wd_hbm, dy_hbm, t_hbm, m_hbm, v_hbm,
    dgu_a, dgu_b, part_ref, far_out, n_out, m_out, v_out,
    w_s, wd_s, dy_s, act_s, dgu_s, t_s, both, recv, send, keep, got, s_d1, far_d1, s_gua, far_gua, n_s, m_s, v_s,
    sems, tile_sems, send_sems, recv_sems, wide_send, wide_recv, x_send, x_recv,
):
    step = pl.program_id(0)
    chip, core, partner = place()
    across = {"dp": 2 * (1 - chip) + core}
    half, tile, last = wd_s.shape[0], a_ref.shape[0], 2 * steps + 2
    own = half // 2
    rows, n = part_ref.shape[0], send.shape[2]
    second = steps + 3

    free = iter([sems.at[k] for k in range(16)])

    def copying(source, target):
        return pltpu.make_async_copy(source, target, next(free))

    def weights(its_chip):
        cols = pl.ds(pl.multiple_of(its_chip * half, 128), half)
        return [
            copying(wg_hbm.at[1, :, cols], w_s.at[:, :half]),
            copying(wu_hbm.at[1, :, cols], w_s.at[:, half:]),
            copying(wd_hbm.at[1, cols, :], wd_s),
        ]

    loads_a, loads_b = weights(1 - chip), weights(chip)
    all_dy, all_t = copying(dy_hbm.at[0], dy_s), copying(t_hbm, t_s)
    block = pl.ds(pl.multiple_of((2 * chip + core) * own, 16), own)
    moments = [copying(wd_hbm.at[1, block, :], n_s), copying(m_hbm.at[1], m_s), copying(v_hbm.at[1], v_s)]
    save_a = copying(dgu_s, dgu_a)
    saves = [copying(n_s, n_out), copying(m_s, m_out), copying(v_s, v_out), copying(far_gua, far_out)]
    cuts = slice(0, 512), slice(512, dy_s.shape[1])
    x_d1 = [to_partner(s_d1.at[:, cut], far_d1.at[:, cut], x_send.at[c], x_recv.at[c], across) for c, cut in enumerate(cuts)]
    x_gua = to_partner(s_gua, far_gua, x_send.at[2], x_recv.at[2], across)

    def save_b(k):
        stretch = pl.ds(pl.multiple_of(k * tile, tile), tile)
        return pltpu.make_async_copy(dgu_s.at[stretch], dgu_b.at[stretch], tile_sems.at[k])

    @pl.when(step == 0)
    def _():
        for load in loads_a:
            load.start()
        barrier = pltpu.get_barrier_semaphore()
        for other in (partner, across):
            pl.semaphore_signal(barrier, inc=1, device_id=other, device_id_type=pl.DeviceIdType.MESH)
        pl.semaphore_wait(barrier, 2)
        for load in loads_a:
            load.wait()
        all_dy.start()
        all_t.start()

    @pl.when(step == steps)
    def _():
        save_a.start()
        for load in loads_b + moments:
            load.start()
        all_t.wait()

    @pl.when(step == second)
    def _():
        for load in loads_b:
            load.wait()
        save_a.wait()

    @pl.when((step < steps) | (step >= second))
    def _():
        k = jnp.where(step < steps, step, step - second)
        stretch = pl.ds(pl.multiple_of(k * tile, tile), tile)
        a, dy = a_ref[...], dy_ref[0]
        hidden = dot(a, w_s[...])
        gate, up = hidden[:, :half], hidden[:, half:]
        d_act = dot(dy, wd_s[...], TURNED).astype(BF16).astype(F32)
        p, slope = silu(gate)
        act_s[stretch, :] = (p * up).astype(BF16)
        dgu_s[stretch, :half] = (d_act * (up * slope)).astype(BF16)
        dgu_s[stretch, half:] = (d_act * p).astype(BF16)

        @pl.when(step >= second)
        def _():
            save_b(k).start()

    @pl.when(step == steps - 1)
    def _():
        all_dy.wait()

    @pl.when((step == steps - 1) | (step == last))
    def _():
        phase = jnp.where(step == last, 1, 0)
        _, their_rows = owned(half, 1 - core)
        _, my_rows = owned(half, core)
        for c, cut in enumerate(cuts):
            copy = to_partner(
                both.at[0, their_rows, cut], recv.at[phase, :, cut], send_sems.at[phase, c], recv_sems.at[phase, c], partner
            )

            @pl.loop(0, 2)
            def _(k):
                cols, _ = owned(half, jnp.where(k == 0, 1 - core, core))
                both[k, :, cut] = dot(act_s[:, cols], dy_s[:, cut], TALL).astype(BF16)

                @pl.when(k == 0)
                def _():
                    copy.start()

            copy.wait()

            @pl.when(step == steps - 1)
            def _():
                s_d1[:, cut] = (both[1, my_rows, cut].astype(F32) + recv[0, :, cut].astype(F32)).astype(BF16)
                x_d1[c].start()

    @pl.when((step >= steps) & (step < second))
    def _():
        k = step - steps

        def copy(k):
            return to_partner(send.at[k], got.at[k], wide_send.at[k], wide_recv.at[k], partner)

        def fold(k):
            copy(k).wait()
            cols = pl.ds(pl.multiple_of(k * n, 128), n)
            s_gua[:, cols] = (keep[k, :rows].astype(F32) + got[k, :rows].astype(F32)).astype(BF16)
            part_ref[:, cols] = keep[k, rows:].astype(F32) + got[k, rows:].astype(F32)

        g = dot(t_s[...], dgu_s[:, pl.ds(pl.multiple_of(k * n, 128), n)]).astype(BF16)
        send[k] = g[: 2 * rows]
        keep[k] = g[2 * rows :]
        copy(k).start()

        @pl.when(k > 0)
        def _():
            fold(k - 1)

        @pl.when(k == 2)
        def _():
            fold(k)
            x_gua.start()

    @pl.when(step == last)
    def _():
        for load in moments:
            load.wait()
        for x in x_d1:
            x.wait()
        skip = core * (own % 128)

        few = 64

        @pl.loop(0, own // few)
        def _(k):
            r = pl.ds(pl.multiple_of(k * few, 16), few)
            mine = both[1, pl.ds(pl.multiple_of(skip + k * few, 16), few), :]
            g = mine.astype(F32) + recv[1, r, :].astype(F32) + far_d1[r, :].astype(F32)
            w, m, v = adamw(n_s[r, :].astype(F32), m_s[r, :], v_s[r, :], g.astype(BF16).astype(F32))
            n_s[r, :] = w
            m_s[r, :] = m
            v_s[r, :] = v

        for save in saves[:3]:
            save.start()
        x_gua.wait()
        saves[3].start()
        for k in range(steps):
            save_b(k).wait()
        for save in saves:
            save.wait()


def wide_body(steps, t_ref, d_ref, out_ref, part_ref, send, keep, recv, send_sem, recv_sem):
    step = pl.program_id(0)
    _, _, partner = place()
    rows, n = out_ref.shape[0], d_ref.shape[1]

    @pl.when(step == 0)
    def _():
        greet(partner)

    def copy(k):
        return to_partner(send.at[k], recv.at[k], send_sem.at[k], recv_sem.at[k], partner)

    def fold(k):
        copy(k).wait()
        cols = pl.ds(pl.multiple_of(k * n, 128), n)
        out_ref[:, cols] = (keep[k, :rows].astype(F32) + recv[k, :rows].astype(F32)).astype(BF16)
        part_ref[:, cols] = keep[k, rows:].astype(F32) + recv[k, rows:].astype(F32)

    g = dot(t_ref[...], d_ref[...]).astype(BF16)
    send[step] = g[: 2 * rows]
    keep[step] = g[2 * rows :]
    copy(step).start()

    @pl.when(step > 0)
    def _():
        fold(step - 1)

    @pl.when(step == steps - 1)
    def _():
        fold(step)


def down_body(act_ref, d_ref, out_ref, part_ref, both, recv, send_sem, recv_sem):
    step = pl.program_id(0)
    chip, core, partner = place()
    half = act_ref.shape[1]
    _, their_rows = owned(half, 1 - core)
    _, my_rows = owned(half, core)

    @pl.when(step == 0)
    def _():
        greet(partner)

    def copy(k):
        return to_partner(both.at[0, k, their_rows], recv.at[k], send_sem.at[k], recv_sem.at[k], partner)

    @pl.loop(0, 2)
    def _(k):
        cols, _ = owned(half, jnp.where(k == 0, 1 - core, core))
        both[k, step] = dot(act_ref[:, cols], d_ref[...], TALL).astype(BF16)

        @pl.when(k == 0)
        def _():
            copy(step).start()

    @pl.when(step == 1)
    def _():
        for k in range(2):
            copy(k).wait()
        out_ref[...] = (both[1, 1 - chip, my_rows, :].astype(F32) + recv[1 - chip].astype(F32)).astype(BF16)
        part_ref[...] = both[1, chip, my_rows, :].astype(F32) + recv[chip].astype(F32)


def back_body(at, da_ref, db_ref, wg_hbm, wu_hbm, h_ref, dy_ref, d_out_ref, w_s, sems):
    step = pl.program_id(0)
    half = da_ref.shape[1] // 2
    loads = []
    for k, w in enumerate((wg_hbm, wu_hbm)):
        for which, chip in enumerate((1 - at[0], at[0])):
            cols = pl.ds(pl.multiple_of(chip * half, 128), half)
            loads.append(pltpu.make_async_copy(w.at[1, :, cols], w_s.at[k, :, which * half : (which + 1) * half], sems.at[k, which]))

    @pl.when(step == 0)
    def _():
        for load in loads:
            load.start()
        for load in loads:
            load.wait()

    chunk = 256
    for lo in range(0, h_ref.shape[0], chunk):
        r = slice(lo, lo + chunk)
        terms = []
        for k in range(2):
            cut = slice(k * half, (k + 1) * half)
            d = jnp.concatenate([da_ref[r, cut], db_ref[r, cut]], axis=1)
            terms.append(dot(w_s[k], d, TURNED).astype(BF16).astype(F32))
        d_a = (terms[0] + terms[1]).T
        h = h_ref[r].astype(F32)
        scale = lax.rsqrt(jnp.mean(h * h, -1, keepdims=True) + 1e-6)
        along = jnp.mean(d_a * h, -1, keepdims=True)
        d_h = (scale * d_a - h * (scale * scale * scale * along)).astype(BF16)
        d_out_ref[r] = (dy_ref[0, r].astype(F32) + d_h.astype(F32)).astype(BF16)


def bottom_body(steps, d_out_ref, t_ref, wd_ref, p_ref, q_ref, out_ref, part_ref, dgu, send, keep, recv, send_sem, recv_sem):
    step = pl.program_id(0)
    _, _, partner = place()
    rows, n = out_ref.shape[0], wd_ref.shape[0]

    @pl.when(step == 0)
    def _():
        greet(partner)

    def copy(k):
        return to_partner(send.at[k], recv.at[k], send_sem.at[k], recv_sem.at[k], partner)

    def fold(k):
        copy(k).wait()
        for p in range(2):
            cut = slice(p * n, (p + 1) * n)
            cols = pl.ds(pl.multiple_of((p * steps + k) * n, 128), n)
            out_ref[:, cols] = (keep[k, :rows, cut].astype(F32) + recv[k, :rows, cut].astype(F32)).astype(BF16)
            part_ref[:, cols] = keep[k, rows:, cut].astype(F32) + recv[k, rows:, cut].astype(F32)

    for lo in range(0, dgu.shape[0], 512):
        stretch = slice(lo, lo + 512)
        d_act = dot(d_out_ref[stretch, :], wd_ref[...], TURNED).astype(BF16).astype(F32)
        dgu[stretch, :n] = (d_act * q_ref[stretch, :]).astype(BF16)
        dgu[stretch, n:] = (d_act * p_ref[stretch, :]).astype(BF16)
    g = dot(t_ref[...], dgu[...]).astype(BF16)
    send[step] = g[: 2 * rows]
    keep[step] = g[2 * rows :]
    copy(step).start()

    @pl.when(step > 0)
    def _():
        fold(step - 1)

    @pl.when(step == steps - 1)
    def _():
        fold(step)


def adamw(w, m, v, g):
    m = 0.9 * m + 0.1 * g
    v = 0.95 * v + 0.05 * g * g
    step = m * lax.rsqrt(v + 1e-8) + 0.1 * w
    return (w - 0.02 * step).astype(BF16), m, v


def adamw_body(parts, n_old, at, part_ref, far_ref, *refs):
    ins, outs = refs[: 3 * parts], refs[3 * parts + n_old :]
    width = part_ref.shape[1] // parts

    @pl.loop(0, part_ref.shape[0] // 16)
    def _(k):
        rows = pl.ds(pl.multiple_of(k * 16, 16), 16)
        for p in range(parts):
            cut = slice(p * width, (p + 1) * width)
            g = (part_ref[rows, cut] + far_ref[rows, cut].astype(F32)).astype(BF16).astype(F32)
            w_ref, m_ref, v_ref = ins[3 * p : 3 * p + 3]
            w, m, v = adamw(w_ref[rows, :].astype(F32), m_ref[rows, :], v_ref[rows, :], g)
            outs[0][rows, cut] = w
            outs[1 + 2 * p][rows, :] = m
            outs[2 + 2 * p][rows, :] = v


def put_body(parts, blocks, n_old, *refs):
    n = len(blocks)
    sources, outs = refs[:n], refs[n + n_old : n + n_old + parts]
    held, in_sems, out_sems = refs[n + n_old + parts :]
    chip, core, _ = place()
    reads = [pltpu.make_async_copy(sources[k], held.at[k], in_sems.at[k]) for k in range(n)]
    for read in reads:
        read.start()
    writes = []
    for k, (layer, far, other, first, half) in enumerate(blocks):
        reads[k].wait()
        rows, width = sources[k].shape
        width //= parts
        its_chip = 1 - chip if far else chip
        its_core = 1 - core if other else core
        own = outs[0].shape[1] // 4
        to_rows = pl.ds(pl.multiple_of((2 * its_chip + its_core) * own + first, 16), rows)
        if half is None:
            to_cols = slice(None)
        elif half is not True and half is not False:
            to_cols = pl.ds(half, width)
        else:
            to_cols = pl.ds(pl.multiple_of((its_chip if half else 1 - its_chip) * width, 128), width)
        for p in range(parts):
            write = pltpu.make_async_copy(
                held.at[k, :, pl.ds(p * width, width)], outs[p].at[layer, to_rows, to_cols], out_sems.at[k, p]
            )
            write.start()
            writes.append(write)
    for write in writes:
        write.wait()


def fill_body(m_ref, v_ref, *refs):
    outs, (held, sems) = refs[-4:-2], refs[-2:]
    reads = [pltpu.make_async_copy(a, held.at[k], sems.at[0, k]) for k, a in enumerate((m_ref, v_ref))]
    writes = [pltpu.make_async_copy(held.at[k], a.at[1], sems.at[1, k]) for k, a in enumerate(outs)]
    for read in reads:
        read.start()
    for read, write in zip(reads, writes):
        read.wait()
        write.start()
    for write in writes:
        write.wait()


def per_device(x, dy, wg, wu, wd, mg, mu, md, vg, vu, vd):
    _, tokens, d = x.shape
    _, _, ff = wg.shape
    half = ff // 2
    place = lax.axis_index("dp")
    chip, core = place // 2, place % 2
    at = jnp.stack([chip, core]).astype(jnp.int32)
    tile = 256
    steps = tokens // tile
    mm = 2 * tokens * d * ff

    def shape(*s, t=BF16):
        return jax.ShapeDtypeStruct(s, t)

    def over_x(value):
        return lax.ppermute(value, "dp", [(0, 2), (1, 3), (2, 0), (3, 1)])

    def over_core(value):
        return lax.ppermute(value, "dp", [(0, 1), (1, 0), (2, 3), (3, 2)])

    rows = lambda i, at: (i, 0)
    seq = spec((1, tile, d), lambda i, at: (0, i, 0))

    n, by = 256, 512
    ff_steps = ff // n
    ff_tile = lambda i: jnp.minimum(i, ff_steps - 1)
    token_tile = lambda i: jnp.maximum(i - ff_steps, 0)
    w_tile = spec((None, d, n), lambda i, at: (0, 0, ff_tile(i)))
    by_ff = spec((tokens, n), lambda i, at: (0, ff_tile(i)))
    by_token = spec((by, d), lambda i, at: (token_tile(i), 0))
    turned = spec((d, by), lambda i, at: (0, token_tile(i)))
    a0t, p0, q0, act0, h1, a1, a1t = call(
        functools.partial(forward_body, ff_steps), at, (x, wg, wu, wd),
        [spec((1, tokens, d), lambda i, at: (0, 0, 0), True), w_tile, w_tile, ANY],
        [shape(d, tokens), shape(tokens, ff, t=F32), shape(tokens, ff, t=F32), shape(tokens, ff), shape(tokens, d), shape(tokens, d), shape(d, tokens)],
        [turned, by_ff, by_ff, by_ff, by_token, by_token, turned], (ff_steps + tokens // by,),
        [pltpu.VMEM((tokens, d), BF16), pltpu.VMEM((tokens, ff), BF16), pltpu.VMEM((ff, d), BF16), pltpu.SemaphoreType.DMA],
        flops=3 * mm, moved=70e6,
    )

    def buffers(slots, rows_sent, rows, n):
        sem = pltpu.SemaphoreType.DMA((slots,))
        return [pltpu.VMEM((slots, rows_sent, n), BF16), pltpu.VMEM((slots, rows_sent, n), BF16), pltpu.VMEM((slots, rows, n), BF16), sem, sem]

    def middle():
        own, r, n = half // 2, d // 4, ff // 3
        tile_at = lambda i: jnp.where(i < steps, i, jnp.maximum(i - steps - 3, 0))
        sem = pltpu.SemaphoreType.DMA
        bf = lambda *s: pltpu.VMEM(s, BF16)
        return call_with_partner(
            functools.partial(middle_body, steps), 0, (a1, dy, wg, wu, wd, dy, a1t, md, vd),
            [spec((tile, d), lambda i: (tile_at(i), 0)), spec((1, tile, d), lambda i: (0, tile_at(i), 0))] + [ANY] * 7,
            [shape(tokens, ff), shape(tokens, ff), shape(r, ff, t=F32), shape(r, ff), shape(own, d), shape(own, d, t=F32), shape(own, d, t=F32)],
            [ANY, ANY, spec((r, ff), CORNER, True)] + [ANY] * 4, (2 * steps + 3,),
            [bf(d, ff), bf(half, d), bf(tokens, d), bf(tokens, half), bf(tokens, ff), bf(d, tokens), bf(2, own + own % 128, d), bf(2, own, d),
             bf(3, 2 * r, n), bf(3, 2 * r, n), bf(3, 2 * r, n), bf(own, d), bf(own, d), bf(r, ff), bf(r, ff), bf(own, d),
             pltpu.VMEM((own, d), F32), pltpu.VMEM((own, d), F32),
             sem((16,)), sem((steps,))] + [sem((2, 2))] * 2 + [sem((3,))] * 4,
            5 * mm, 60e6, (), 63,
        )

    def wide(identity, t, dgu, after):
        n, r = ff // 3, d // 4
        full = spec((r, ff), CORNER, True)
        return call_with_partner(
            functools.partial(wide_body, 3), identity, (t, dgu), [spec((d, tokens), CORNER, True), spec((tokens, n), lambda i: (0, i))],
            [shape(r, ff), shape(r, ff, t=F32)], [full, full], (3,), buffers(3, 2 * r, 2 * r, n), mm, 17e6, after,
        )

    def update(part, far, layer, parts, cols, old, after=(), stretch=(0, 2)):
        n_rows, n_cols = part.shape
        width = n_cols // len(parts)
        first, n = stretch
        tiles = 2
        tile_r = n_rows // tiles
        flat = spec((tile_r, n_cols), lambda i, at: (first + i, 0))
        specs, args = [flat, flat], [part, far]
        outs, out_specs = [shape(n * tile_r, n_cols)], [spec((tile_r, n_cols), rows)]
        for w, m, v in parts:
            local = spec((None, tile_r, width), lambda i, at: (layer, first + i, cols(at)))
            specs += [spec((None, tile_r, width), lambda i, at: (layer, (2 * at[0] + at[1]) * tiles + first + i, cols(at))), local, local]
            args += [w, m, v]
            outs += [shape(*m.shape, t=F32)] * 2
            out_specs += [local, local]
        aliases = {}
        for k, o in enumerate(old):
            aliases[len(args)] = 1 + k
            args.append(o)
            specs.append(ANY)
        got = call(
            functools.partial(adamw_body, len(parts), len(old)), at, args, specs, outs, out_specs, (n,),
            aliases=aliases, flops=20e6, moved=20 * n_rows * n_cols, after=after,
        )
        return got[0], got[1:]

    def put(sources, blocks, shapes, old, after=()):
        n, parts = len(sources), len(shapes)
        args = list(sources) + list(old) + list(after)
        return pl.pallas_call(
            lambda *refs: put_body(parts, blocks, len(old) + len(after), *refs),
            in_specs=[ANY] * len(args),
            out_specs=[ANY] * parts,
            out_shape=[shape(*s) for s in shapes],
            scratch_shapes=[pltpu.VMEM((n, *sources[0].shape), BF16), pltpu.SemaphoreType.DMA((n,)), pltpu.SemaphoreType.DMA((n, parts))],
            input_output_aliases={n + k: k for k in range(len(old))},
            compiler_params=pltpu.CompilerParams(vmem_limit_bytes=60 * MIB),
            cost_estimate=pl.CostEstimate(flops=1000000, bytes_accessed=4000000 * n, transcendentals=0),
        )(*args)

    def put_all(new, far, layer, half, shapes, old, after=()):
        blocks = [(layer, f, o, 0, half) for f in (False, True) for o in (False, True)]
        return put([new, over_core(new), far, over_core(far)], blocks, shapes, old, after)

    none = lambda at: 0
    cols_a, cols_b = (lambda at: 1 - at[0]), (lambda at: at[0])
    gu = [(wg, mg, vg), (wu, mu, vu)]
    r = ff // 4

    dgu_a, dgu_b, part_gua, far_gua, n_d1, m_d1, v_d1 = middle()
    all_d1 = over_x(n_d1)
    s, part_gub = wide(3, a1t, dgu_b, [n_d1])
    far_gub = over_x(s)
    n_gub, old_gu = update(part_gub, far_gua, 1, gu, cols_b, [])
    all_gub = over_x(n_gub)

    wide_tile = 512
    by_rows = lambda n: spec((wide_tile, n), rows)
    d_out = call(
        back_body, at, (dgu_a, dgu_b, wg, wu, h1, dy),
        [by_rows(ff), by_rows(ff), ANY, ANY, by_rows(d), spec((1, wide_tile, d), lambda i, at: (0, i, 0))],
        shape(tokens, d), by_rows(d), (tokens // wide_tile,), [pltpu.VMEM((2, d, ff), BF16), pltpu.SemaphoreType.DMA((2, 2))], flops=2 * mm, moved=35e6, after=[n_gub],
    )

    def bottom(identity, first, steps, after):
        n, r = 256, d // 4
        cols = 2 * n * steps
        full = spec((r, cols), CORNER, True)
        to_cols = spec((tokens, n), lambda i: (0, first + i))
        return call_with_partner(
            functools.partial(bottom_body, steps), identity, (d_out, a0t, wd, p0, q0),
            [spec((tokens, d), CORNER, True), spec((d, tokens), CORNER, True),
             spec((None, n, d), lambda i: (0, first + i, 0)), to_cols, to_cols],
            [shape(r, cols), shape(r, cols, t=F32)], [full, full], (steps,),
            [pltpu.VMEM((tokens, 2 * n), BF16)] + buffers(steps, 2 * r, 2 * r, 2 * n),
            3 * mm * steps // 9, 50e6 * steps / 9, after,
        )

    n_gua, old_gu = update(part_gua, far_gub, 1, gu, cols_a, old_gu, [d_out])
    all_gua = over_x(n_gua)
    full = spec((r, d), CORNER, True)
    s, part_d0 = call_with_partner(
        down_body, 4, (act0, d_out), [spec((tokens, half), lambda i: (0, i)), spec((tokens, d), CORNER, True)],
        [shape(r, d), shape(r, d, t=F32)], [full, full], (2,), [pltpu.VMEM((2, 2, r + r % 128, d), BF16), pltpu.VMEM((2, r, d), BF16)] + [pltpu.SemaphoreType.DMA((2,))] * 2, mm, 17e6, [n_gua],
    )
    far_d0 = over_x(s)
    s, part_0 = bottom(5, 0, 6, [s])
    far_0 = over_x(s)
    s, part_1 = bottom(6, 6, 3, [s])
    far_1 = over_x(s)
    n_d0, new_d = update(part_d0, far_d0, 0, [(wd, md, vd)], none, [], [s])
    all_d0 = over_x(n_d0)
    both = [wg.shape, wu.shape]
    out_d = put_all(n_d1, all_d1, 1, None, [wd.shape], [], [n_d0])
    out_gu = put_all(n_gub, all_gub, 1, True, both, [], out_d)
    n_0, old_gu = update(part_0, far_0, 0, gu, none, old_gu, out_gu[:1])
    all_0 = over_x(n_0)
    out_gu = put_all(n_gua, all_gua, 1, False, both, out_gu, [n_0])
    third = lambda at: 2
    n_top, old_gu = update(part_1, far_1, 0, gu, third, old_gu, out_gu[:1], (0, 1))
    far_top = over_x(n_top)
    n_low, (mg, vg, mu, vu) = update(part_1, far_1, 0, gu, third, old_gu, [n_top], (1, 1))
    far_low = over_x(n_low)
    new_d = pl.pallas_call(
        fill_body,
        in_specs=[ANY] * 5,
        out_specs=[ANY] * 2,
        out_shape=[shape(*md.shape, t=F32)] * 2,
        scratch_shapes=[pltpu.VMEM((2, *m_d1.shape), F32), pltpu.SemaphoreType.DMA((2, 2))],
        input_output_aliases={2: 0, 3: 1},
        compiler_params=pltpu.CompilerParams(vmem_limit_bytes=60 * MIB),
        cost_estimate=pl.CostEstimate(flops=1000000, bytes_accessed=8000000, transcendentals=0),
        name="fill_d",
    )(m_d1, v_d1, *new_d, n_low)
    out_d = put_all(n_d0, all_d0, 0, None, [wd.shape], out_d, [n_low])
    first = n_top.shape[0]
    start = part_0.shape[1] // 2
    blocks = [(0, f, o, low, start) for f in (False, True) for low in (0, first) for o in (False, True)]
    out_gu = put([n_top, over_core(n_top), n_low, over_core(n_low)], blocks[:4], both, out_gu, out_d)
    out_gu = put_all(n_0, all_0, 0, 0, both, out_gu)
    out_gu = put([far_top, over_core(far_top)], blocks[4:6], both, out_gu)
    out_gu = put([far_low, over_core(far_low)], blocks[6:], both, out_gu)
    return out_gu[0], out_gu[1], out_d[0], mg, mu, new_d[0], vg, vu, new_d[1]


def solution(mesh):
    whole, part = P(None, None, None), P(None, "dp", None)
    seqs = P(("rep", "dp"), None, None)

    return jax.shard_map(
        per_device,
        mesh=mesh,
        in_specs=(seqs, seqs, whole, whole, whole) + (part,) * 6,
        out_specs=(P("rep", None, None),) * 3 + (P("rep", "dp", None),) * 6,
        check_vma=False,
    )
```

```python
import functools

import jax
import jax.numpy as jnp
from jax import lax
from jax.experimental import pallas as pl
from jax.experimental.pallas import tpu as pltpu
from jax.sharding import PartitionSpec as P


F32, BF16 = jnp.float32, jnp.bfloat16
MIB = 2**20


def dot(a, b, contract=((1,), (0,))):
    return lax.dot_general(a, b, (contract, ((), ())), preferred_element_type=F32)


def normed(h):
    scale = lax.rsqrt(jnp.mean(h * h, -1, keepdims=True) + 1e-6)
    return (h * scale).astype(BF16), scale


def call(body, at, args, specs, outs, out_specs, grid, scratch=(), aliases=None, flops=0, moved=0, after=(), vmem=60):
    n = len(args)
    args, specs = list(args) + list(after), list(specs) + [ANY] * len(after)
    return pl.pallas_call(
        lambda at, *refs: body(at, *refs[:n], *refs[n + len(after) :]),
        grid_spec=pltpu.PrefetchScalarGridSpec(
            num_scalar_prefetch=1, grid=grid, in_specs=specs, out_specs=out_specs, scratch_shapes=list(scratch)
        ),
        out_shape=outs,
        input_output_aliases={k + 1: v for k, v in (aliases or {}).items()},
        compiler_params=pltpu.CompilerParams(
            dimension_semantics=("arbitrary",) * len(grid), vmem_limit_bytes=vmem * MIB
        ),
        cost_estimate=pl.CostEstimate(flops=int(flops), bytes_accessed=int(moved), transcendentals=0),
    )(at, *args)


def call_with_partner(body, identity, args, specs, outs, out_specs, grid, scratch, flops, moved, after=(), vmem=60):
    n = len(args)
    args, specs = list(args) + list(after), list(specs) + [ANY] * len(after)
    return pl.pallas_call(
        lambda *refs: body(*refs[:n], *refs[n + len(after) :]),
        grid=grid,
        in_specs=specs,
        out_specs=out_specs,
        scratch_shapes=list(scratch),
        out_shape=outs,
        compiler_params=pltpu.CompilerParams(
            dimension_semantics=("arbitrary",) * len(grid), vmem_limit_bytes=vmem * MIB,
            collective_id=identity, has_side_effects=True,
        ),
        cost_estimate=pl.CostEstimate(flops=int(flops), bytes_accessed=int(moved), transcendentals=0),
    )(*args)


def place():
    at = lax.axis_index("dp")
    chip, core = at // 2, at % 2
    return chip, core, {"dp": 2 * chip + 1 - core}


def greet(partner):
    barrier = pltpu.get_barrier_semaphore()
    pl.semaphore_signal(barrier, inc=1, device_id=partner, device_id_type=pl.DeviceIdType.MESH)
    pl.semaphore_wait(barrier, 1)


def to_partner(source, target, send_sem, recv_sem, partner):
    return pltpu.make_async_remote_copy(
        source, target, send_sem, recv_sem, device_id=partner, device_id_type=pl.DeviceIdType.MESH
    )


def spec(shape, index, once=False):
    if once:
        return pl.BlockSpec(shape, index, pipeline_mode=pl.Buffered(1))
    return pl.BlockSpec(shape, index)


ANY = pl.BlockSpec(memory_space=pl.ANY)
TURNED, TALL = ((1,), (1,)), ((0,), (0,))


def CORNER(*_):
    return 0, 0


def silu(gate):
    t = 0.5 * jnp.tanh(0.5 * gate)
    s = 0.5 + t
    p = gate * s
    return p, s + p * (0.5 - t)


def store_transposed(at, a, to):
    turned = a.T
    rows = turned.shape[0] // 4
    for owner in range(4):
        place = 2 * jnp.where(at[1] == owner % 2, 1, 0) + jnp.where(at[0] == owner // 2, 1, 0)
        to[pl.ds(pl.multiple_of(place * rows, rows), rows), :] = turned[owner * rows : (owner + 1) * rows]


def forward_body(
    ff_steps, at, x_ref, wg_ref, wu_ref, wd_hbm, a0t_ref, p_ref, q_ref, act_ref, h_ref, a1_ref, a1t_ref, a_s, act_s, wd_s, sem
):
    step = pl.program_id(0)
    tokens, n, tile, chunk = a_s.shape[0], wg_ref.shape[1], h_ref.shape[0], 256
    load = pltpu.make_async_copy(wd_hbm.at[0], wd_s, sem)

    def hidden(fresh, los):
        cols = slice(0, n) if fresh else pl.ds(pl.multiple_of(step * n, n), n)
        for lo in los:
            r = pl.ds(lo, chunk)
            if fresh:
                a, _ = normed(x_ref[0, r].astype(F32))
                a_s[r] = a
            else:
                a = a_s[r]
            gate, up = dot(a, wg_ref[...]), dot(a, wu_ref[...])
            p, slope = silu(gate)
            p_ref[r] = p
            q_ref[r] = up * slope
            act = (p * up).astype(BF16)
            act_ref[r] = act
            act_s[r, cols] = act

    @pl.when(step == 0)
    def _():
        load.start()
        hidden(True, range(0, tokens, chunk))

    @pl.when((step > 0) & (step < ff_steps))
    def _():
        hidden(False, range(0, tokens, chunk))

    @pl.when(step == ff_steps)
    def _():
        load.wait()

    @pl.when(step >= ff_steps)
    def _():
        base = (step - ff_steps) * tile
        for lo in range(0, tile, chunk):
            r = pl.ds(pl.multiple_of(base + lo, chunk), chunk)
            to = slice(lo, lo + chunk)
            out = dot(act_s[r], wd_s[...]).astype(BF16)
            h = (x_ref[0, r].astype(F32) + out.astype(F32)).astype(BF16)
            h_ref[to] = h
            a1_ref[to] = normed(h.astype(F32))[0]
        store_transposed(at, a1_ref[...], a1t_ref)
        store_transposed(at, a_s[pl.ds(pl.multiple_of(base, tile), tile)], a0t_ref)


def owned(half, core):
    own = half // 2
    extra = own % 128
    start = core * (own - extra)
    return pl.ds(pl.multiple_of(start, 128), own + extra), pl.ds(pl.multiple_of(core * extra, 16), own)


def middle_body(
    steps, a_ref, dy_ref, wg_hbm, wu_hbm, wd_hbm, dy_hbm, t_hbm, m_hbm, v_hbm,
    dgu_a, dgu_b, part_ref, far_out, n_out, m_out, v_out,
    w_s, wd_s, dy_s, act_s, dgu_s, t_s, both, recv, send, keep, got, s_d1, far_d1, s_gua, n_s, m_s, v_s,
    sems, tile_sems, send_sems, recv_sems, wide_send, wide_recv, x_send, x_recv,
):
    step = pl.program_id(0)
    chip, core, partner = place()
    across = {"dp": 2 * (1 - chip) + core}
    half, tile, last = wd_s.shape[0], a_ref.shape[0], 2 * steps + 2
    own = half // 2
    rows, n = part_ref.shape[0], send.shape[2]
    second = steps + 3

    free = iter([sems.at[k] for k in range(16)])

    def copying(source, target):
        return pltpu.make_async_copy(source, target, next(free))

    def weights(its_chip):
        cols = pl.ds(pl.multiple_of(its_chip * half, 128), half)
        return [
            copying(wg_hbm.at[1, :, cols], w_s.at[:, :half]),
            copying(wu_hbm.at[1, :, cols], w_s.at[:, half:]),
            copying(wd_hbm.at[1, cols, :], wd_s),
        ]

    loads_a, loads_b = weights(1 - chip), weights(chip)
    all_dy, all_t = copying(dy_hbm.at[0], dy_s), copying(t_hbm, t_s)
    block = pl.ds(pl.multiple_of((2 * chip + core) * own, 16), own)
    moments = [copying(wd_hbm.at[1, block, :], n_s), copying(m_hbm.at[1], m_s), copying(v_hbm.at[1], v_s)]
    save_a = copying(dgu_s, dgu_a)
    saves = [copying(n_s, n_out), copying(m_s, m_out), copying(v_s, v_out)]
    cuts = slice(0, 512), slice(512, dy_s.shape[1])
    x_d1 = [to_partner(s_d1.at[:, cut], far_d1.at[:, cut], x_send.at[c], x_recv.at[c], across) for c, cut in enumerate(cuts)]
    x_gua = to_partner(s_gua, far_out, x_send.at[2], x_recv.at[2], across)

    def save_b(k):
        stretch = pl.ds(pl.multiple_of(k * tile, tile), tile)
        return pltpu.make_async_copy(dgu_s.at[stretch], dgu_b.at[stretch], tile_sems.at[k])

    @pl.when(step == 0)
    def _():
        for load in loads_a:
            load.start()
        barrier = pltpu.get_barrier_semaphore()
        for other in (partner, across):
            pl.semaphore_signal(barrier, inc=1, device_id=other, device_id_type=pl.DeviceIdType.MESH)
        pl.semaphore_wait(barrier, 2)
        for load in loads_a:
            load.wait()
        all_dy.start()
        all_t.start()

    @pl.when(step == steps)
    def _():
        save_a.start()
        for load in loads_b + moments:
            load.start()
        all_t.wait()

    @pl.when(step == second)
    def _():
        for load in loads_b:
            load.wait()
        save_a.wait()

    @pl.when((step < steps) | (step >= second))
    def _():
        k = jnp.where(step < steps, step, step - second)
        stretch = pl.ds(pl.multiple_of(k * tile, tile), tile)
        a, dy = a_ref[...], dy_ref[0]
        hidden = dot(a, w_s[...])
        gate, up = hidden[:, :half], hidden[:, half:]
        d_act = dot(dy, wd_s[...], TURNED).astype(BF16).astype(F32)
        p, slope = silu(gate)
        act_s[stretch, :] = (p * up).astype(BF16)
        dgu_s[stretch, :half] = (d_act * (up * slope)).astype(BF16)
        dgu_s[stretch, half:] = (d_act * p).astype(BF16)

        @pl.when(step >= second)
        def _():
            save_b(k).start()

    @pl.when(step == steps - 1)
    def _():
        all_dy.wait()

    @pl.when((step == steps - 1) | (step == last))
    def _():
        phase = jnp.where(step == last, 1, 0)
        _, their_rows = owned(half, 1 - core)
        _, my_rows = owned(half, core)
        for c, cut in enumerate(cuts):
            copy = to_partner(
                both.at[0, their_rows, cut], recv.at[phase, :, cut], send_sems.at[phase, c], recv_sems.at[phase, c], partner
            )

            @pl.loop(0, 2)
            def _(k):
                cols, _ = owned(half, jnp.where(k == 0, 1 - core, core))
                both[k, :, cut] = dot(act_s[:, cols], dy_s[:, cut], TALL).astype(BF16)

                @pl.when(k == 0)
                def _():
                    copy.start()

            copy.wait()

            @pl.when(step == steps - 1)
            def _():
                s_d1[:, cut] = (both[1, my_rows, cut].astype(F32) + recv[0, :, cut].astype(F32)).astype(BF16)
                x_d1[c].start()

    @pl.when((step >= steps) & (step < second))
    def _():
        k = step - steps

        def copy(k):
            return to_partner(send.at[k], got.at[k], wide_send.at[k], wide_recv.at[k], partner)

        def fold(k):
            copy(k).wait()
            cols = pl.ds(pl.multiple_of(k * n, 128), n)
            s_gua[:, cols] = (keep[k, :rows].astype(F32) + got[k, :rows].astype(F32)).astype(BF16)
            part_ref[:, cols] = keep[k, rows:].astype(F32) + got[k, rows:].astype(F32)

        g = dot(t_s[...], dgu_s[:, pl.ds(pl.multiple_of(k * n, 128), n)]).astype(BF16)
        send[k] = g[: 2 * rows]
        keep[k] = g[2 * rows :]
        copy(k).start()

        @pl.when(k > 0)
        def _():
            fold(k - 1)

        @pl.when(k == 2)
        def _():
            fold(k)
            x_gua.start()

    @pl.when(step == last)
    def _():
        for load in moments:
            load.wait()
        for x in x_d1:
            x.wait()
        skip = core * (own % 128)

        few = 64

        @pl.loop(0, own // few)
        def _(k):
            r = pl.ds(pl.multiple_of(k * few, 16), few)
            mine = both[1, pl.ds(pl.multiple_of(skip + k * few, 16), few), :]
            g = mine.astype(F32) + recv[1, r, :].astype(F32) + far_d1[r, :].astype(F32)
            w, m, v = adamw(n_s[r, :].astype(F32), m_s[r, :], v_s[r, :], g.astype(BF16).astype(F32))
            n_s[r, :] = w
            m_s[r, :] = m
            v_s[r, :] = v

        for save in saves:
            save.start()
        x_gua.wait()
        for k in range(steps):
            save_b(k).wait()
        for save in saves:
            save.wait()


def wide_body(steps, t_ref, d_ref, out_ref, part_ref, send, keep, recv, send_sem, recv_sem):
    step = pl.program_id(0)
    _, _, partner = place()
    rows, n = out_ref.shape[0], d_ref.shape[1]

    @pl.when(step == 0)
    def _():
        greet(partner)

    def copy(k):
        return to_partner(send.at[k], recv.at[k], send_sem.at[k], recv_sem.at[k], partner)

    def fold(k):
        copy(k).wait()
        cols = pl.ds(pl.multiple_of(k * n, 128), n)
        out_ref[:, cols] = (keep[k, :rows].astype(F32) + recv[k, :rows].astype(F32)).astype(BF16)
        part_ref[:, cols] = keep[k, rows:].astype(F32) + recv[k, rows:].astype(F32)

    g = dot(t_ref[...], d_ref[...]).astype(BF16)
    send[step] = g[: 2 * rows]
    keep[step] = g[2 * rows :]
    copy(step).start()

    @pl.when(step > 0)
    def _():
        fold(step - 1)

    @pl.when(step == steps - 1)
    def _():
        fold(step)


def down_body(act_ref, d_ref, out_ref, part_ref, both, recv, send_sem, recv_sem):
    step = pl.program_id(0)
    chip, core, partner = place()
    half = act_ref.shape[1]
    _, their_rows = owned(half, 1 - core)
    _, my_rows = owned(half, core)

    @pl.when(step == 0)
    def _():
        greet(partner)

    def copy(k):
        return to_partner(both.at[0, k, their_rows], recv.at[k], send_sem.at[k], recv_sem.at[k], partner)

    @pl.loop(0, 2)
    def _(k):
        cols, _ = owned(half, jnp.where(k == 0, 1 - core, core))
        both[k, step] = dot(act_ref[:, cols], d_ref[...], TALL).astype(BF16)

        @pl.when(k == 0)
        def _():
            copy(step).start()

    @pl.when(step == 1)
    def _():
        for k in range(2):
            copy(k).wait()
        out_ref[...] = (both[1, 1 - chip, my_rows, :].astype(F32) + recv[1 - chip].astype(F32)).astype(BF16)
        part_ref[...] = both[1, chip, my_rows, :].astype(F32) + recv[chip].astype(F32)


def back_body(at, da_ref, db_ref, wg_hbm, wu_hbm, h_ref, dy_ref, d_out_ref, w_s, sems):
    step = pl.program_id(0)
    half = da_ref.shape[1] // 2
    loads = []
    for k, w in enumerate((wg_hbm, wu_hbm)):
        for which, chip in enumerate((1 - at[0], at[0])):
            cols = pl.ds(pl.multiple_of(chip * half, 128), half)
            loads.append(pltpu.make_async_copy(w.at[1, :, cols], w_s.at[k, :, which * half : (which + 1) * half], sems.at[k, which]))

    @pl.when(step == 0)
    def _():
        for load in loads:
            load.start()
        for load in loads:
            load.wait()

    chunk = 256
    for lo in range(0, h_ref.shape[0], chunk):
        r = slice(lo, lo + chunk)
        terms = []
        for k in range(2):
            cut = slice(k * half, (k + 1) * half)
            d = jnp.concatenate([da_ref[r, cut], db_ref[r, cut]], axis=1)
            terms.append(dot(w_s[k], d, TURNED).astype(BF16).astype(F32))
        d_a = (terms[0] + terms[1]).T
        h = h_ref[r].astype(F32)
        scale = lax.rsqrt(jnp.mean(h * h, -1, keepdims=True) + 1e-6)
        along = jnp.mean(d_a * h, -1, keepdims=True)
        d_h = (scale * d_a - h * (scale * scale * scale * along)).astype(BF16)
        d_out_ref[r] = (dy_ref[0, r].astype(F32) + d_h.astype(F32)).astype(BF16)


def bottom_body(steps, d_out_ref, t_ref, wd_ref, p_ref, q_ref, out_ref, part_ref, dgu, send, keep, recv, send_sem, recv_sem):
    step = pl.program_id(0)
    _, _, partner = place()
    rows, n = out_ref.shape[0], wd_ref.shape[0]

    @pl.when(step == 0)
    def _():
        greet(partner)

    def copy(k):
        return to_partner(send.at[k], recv.at[k], send_sem.at[k], recv_sem.at[k], partner)

    def fold(k):
        copy(k).wait()
        for p in range(2):
            cut = slice(p * n, (p + 1) * n)
            cols = pl.ds(pl.multiple_of((p * steps + k) * n, 128), n)
            out_ref[:, cols] = (keep[k, :rows, cut].astype(F32) + recv[k, :rows, cut].astype(F32)).astype(BF16)
            part_ref[:, cols] = keep[k, rows:, cut].astype(F32) + recv[k, rows:, cut].astype(F32)

    for lo in range(0, dgu.shape[0], 512):
        stretch = slice(lo, lo + 512)
        d_act = dot(d_out_ref[stretch, :], wd_ref[...], TURNED).astype(BF16).astype(F32)
        dgu[stretch, :n] = (d_act * q_ref[stretch, :]).astype(BF16)
        dgu[stretch, n:] = (d_act * p_ref[stretch, :]).astype(BF16)
    g = dot(t_ref[...], dgu[...]).astype(BF16)
    send[step] = g[: 2 * rows]
    keep[step] = g[2 * rows :]
    copy(step).start()

    @pl.when(step > 0)
    def _():
        fold(step - 1)

    @pl.when(step == steps - 1)
    def _():
        fold(step)


def adamw(w, m, v, g):
    m = 0.9 * m + 0.1 * g
    v = 0.95 * v + 0.05 * g * g
    step = m * lax.rsqrt(v + 1e-8) + 0.1 * w
    return (w - 0.02 * step).astype(BF16), m, v


def adamw_body(parts, n_old, at, part_ref, far_ref, *refs):
    ins, outs = refs[: 3 * parts], refs[3 * parts + n_old :]
    width = part_ref.shape[1] // parts

    @pl.loop(0, part_ref.shape[0] // 16)
    def _(k):
        rows = pl.ds(pl.multiple_of(k * 16, 16), 16)
        for p in range(parts):
            cut = slice(p * width, (p + 1) * width)
            g = (part_ref[rows, cut] + far_ref[rows, cut].astype(F32)).astype(BF16).astype(F32)
            w_ref, m_ref, v_ref = ins[3 * p : 3 * p + 3]
            w, m, v = adamw(w_ref[rows, :].astype(F32), m_ref[rows, :], v_ref[rows, :], g)
            outs[0][rows, cut] = w
            outs[1 + 2 * p][rows, :] = m
            outs[2 + 2 * p][rows, :] = v


def put_body(parts, blocks, n_old, *refs):
    n = len(blocks)
    sources, outs = refs[:n], refs[n + n_old : n + n_old + parts]
    held, in_sems, out_sems = refs[n + n_old + parts :]
    chip, core, _ = place()
    reads = [pltpu.make_async_copy(sources[k], held.at[k], in_sems.at[k]) for k in range(n)]
    for read in reads:
        read.start()
    writes = []
    for k, (layer, far, other, first, half) in enumerate(blocks):
        reads[k].wait()
        rows, width = sources[k].shape
        width //= parts
        its_chip = 1 - chip if far else chip
        its_core = 1 - core if other else core
        own = outs[0].shape[1] // 4
        to_rows = pl.ds(pl.multiple_of((2 * its_chip + its_core) * own + first, 16), rows)
        if half is None:
            to_cols = slice(None)
        elif half is not True and half is not False:
            to_cols = pl.ds(half, width)
        else:
            to_cols = pl.ds(pl.multiple_of((its_chip if half else 1 - its_chip) * width, 128), width)
        for p in range(parts):
            write = pltpu.make_async_copy(
                held.at[k, :, pl.ds(p * width, width)], outs[p].at[layer, to_rows, to_cols], out_sems.at[k, p]
            )
            write.start()
            writes.append(write)
    for write in writes:
        write.wait()


def fill_body(m_ref, v_ref, *refs):
    outs, (held, sems) = refs[-4:-2], refs[-2:]
    reads = [pltpu.make_async_copy(a, held.at[k], sems.at[0, k]) for k, a in enumerate((m_ref, v_ref))]
    writes = [pltpu.make_async_copy(held.at[k], a.at[1], sems.at[1, k]) for k, a in enumerate(outs)]
    for read in reads:
        read.start()
    for read, write in zip(reads, writes):
        read.wait()
        write.start()
    for write in writes:
        write.wait()


def per_device(x, dy, wg, wu, wd, mg, mu, md, vg, vu, vd):
    _, tokens, d = x.shape
    _, _, ff = wg.shape
    half = ff // 2
    place = lax.axis_index("dp")
    chip, core = place // 2, place % 2
    at = jnp.stack([chip, core]).astype(jnp.int32)
    tile = 256
    steps = tokens // tile
    mm = 2 * tokens * d * ff

    def shape(*s, t=BF16):
        return jax.ShapeDtypeStruct(s, t)

    def over_x(value):
        return lax.ppermute(value, "dp", [(0, 2), (1, 3), (2, 0), (3, 1)])

    def over_core(value):
        return lax.ppermute(value, "dp", [(0, 1), (1, 0), (2, 3), (3, 2)])

    rows = lambda i, at: (i, 0)
    seq = spec((1, tile, d), lambda i, at: (0, i, 0))

    n, by = 256, 512
    ff_steps = ff // n
    ff_tile = lambda i: jnp.minimum(i, ff_steps - 1)
    token_tile = lambda i: jnp.maximum(i - ff_steps, 0)
    w_tile = spec((None, d, n), lambda i, at: (0, 0, ff_tile(i)))
    by_ff = spec((tokens, n), lambda i, at: (0, ff_tile(i)))
    by_token = spec((by, d), lambda i, at: (token_tile(i), 0))
    turned = spec((d, by), lambda i, at: (0, token_tile(i)))
    a0t, p0, q0, act0, h1, a1, a1t = call(
        functools.partial(forward_body, ff_steps), at, (x, wg, wu, wd),
        [spec((1, tokens, d), lambda i, at: (0, 0, 0), True), w_tile, w_tile, ANY],
        [shape(d, tokens), shape(tokens, ff, t=F32), shape(tokens, ff, t=F32), shape(tokens, ff), shape(tokens, d), shape(tokens, d), shape(d, tokens)],
        [turned, by_ff, by_ff, by_ff, by_token, by_token, turned], (ff_steps + tokens // by,),
        [pltpu.VMEM((tokens, d), BF16), pltpu.VMEM((tokens, ff), BF16), pltpu.VMEM((ff, d), BF16), pltpu.SemaphoreType.DMA],
        flops=3 * mm, moved=70e6,
    )

    def buffers(slots, rows_sent, rows, n):
        sem = pltpu.SemaphoreType.DMA((slots,))
        return [pltpu.VMEM((slots, rows_sent, n), BF16), pltpu.VMEM((slots, rows_sent, n), BF16), pltpu.VMEM((slots, rows, n), BF16), sem, sem]

    def middle():
        own, r, n = half // 2, d // 4, ff // 3
        tile_at = lambda i: jnp.where(i < steps, i, jnp.maximum(i - steps - 3, 0))
        sem = pltpu.SemaphoreType.DMA
        bf = lambda *s: pltpu.VMEM(s, BF16)
        return call_with_partner(
            functools.partial(middle_body, steps), 0, (a1, dy, wg, wu, wd, dy, a1t, md, vd),
            [spec((tile, d), lambda i: (tile_at(i), 0)), spec((1, tile, d), lambda i: (0, tile_at(i), 0))] + [ANY] * 7,
            [shape(tokens, ff), shape(tokens, ff), shape(r, ff, t=F32), shape(r, ff), shape(own, d), shape(own, d, t=F32), shape(own, d, t=F32)],
            [ANY, ANY, spec((r, ff), CORNER, True)] + [ANY] * 4, (2 * steps + 3,),
            [bf(d, ff), bf(half, d), bf(tokens, d), bf(tokens, half), bf(tokens, ff), bf(d, tokens), bf(2, own + own % 128, d), bf(2, own, d),
             bf(3, 2 * r, n), bf(3, 2 * r, n), bf(3, 2 * r, n), bf(own, d), bf(own, d), bf(r, ff), bf(own, d),
             pltpu.VMEM((own, d), F32), pltpu.VMEM((own, d), F32),
             sem((16,)), sem((steps,))] + [sem((2, 2))] * 2 + [sem((3,))] * 4,
            5 * mm, 60e6, (), 63,
        )

    def wide(identity, t, dgu, after):
        n, r = ff // 3, d // 4
        full = spec((r, ff), CORNER, True)
        return call_with_partner(
            functools.partial(wide_body, 3), identity, (t, dgu), [spec((d, tokens), CORNER, True), spec((tokens, n), lambda i: (0, i))],
            [shape(r, ff), shape(r, ff, t=F32)], [full, full], (3,), buffers(3, 2 * r, 2 * r, n), mm, 17e6, after,
        )

    def update(part, far, layer, parts, cols, old, after=(), tiles=2, stretch=None):
        n_rows, n_cols = part.shape
        width = n_cols // len(parts)
        first, n = stretch or (0, tiles)
        tile_r = n_rows // tiles
        flat = spec((tile_r, n_cols), lambda i, at: (first + i, 0))
        specs, args = [flat, flat], [part, far]
        outs, out_specs = [shape(n * tile_r, n_cols)], [spec((tile_r, n_cols), rows)]
        for w, m, v in parts:
            if isinstance(cols, int):
                sizes = None, pl.Element(tile_r), pl.Element(width)
                local = spec(sizes, lambda i, at: (layer, (first + i) * tile_r, cols))
                block = spec(sizes, lambda i, at: (layer, ((2 * at[0] + at[1]) * tiles + first + i) * tile_r, cols))
            else:
                local = spec((None, tile_r, width), lambda i, at: (layer, first + i, cols(at)))
                block = spec((None, tile_r, width), lambda i, at: (layer, (2 * at[0] + at[1]) * tiles + first + i, cols(at)))
            specs += [block, local, local]
            args += [w, m, v]
            outs += [shape(*m.shape, t=F32)] * 2
            out_specs += [local, local]
        aliases = {}
        for k, o in enumerate(old):
            aliases[len(args)] = 1 + k
            args.append(o)
            specs.append(ANY)
        got = call(
            functools.partial(adamw_body, len(parts), len(old)), at, args, specs, outs, out_specs, (n,),
            aliases=aliases, flops=20e6, moved=20 * n_rows * n_cols, after=after,
        )
        return got[0], got[1:]

    def put(sources, blocks, shapes, old, after=()):
        n, parts = len(sources), len(shapes)
        args = list(sources) + list(old) + list(after)
        return pl.pallas_call(
            lambda *refs: put_body(parts, blocks, len(old) + len(after), *refs),
            in_specs=[ANY] * len(args),
            out_specs=[ANY] * parts,
            out_shape=[shape(*s) for s in shapes],
            scratch_shapes=[pltpu.VMEM((n, *sources[0].shape), BF16), pltpu.SemaphoreType.DMA((n,)), pltpu.SemaphoreType.DMA((n, parts))],
            input_output_aliases={n + k: k for k in range(len(old))},
            compiler_params=pltpu.CompilerParams(vmem_limit_bytes=60 * MIB),
            cost_estimate=pl.CostEstimate(flops=1000000, bytes_accessed=4000000 * n, transcendentals=0),
        )(*args)

    def put_all(new, far, layer, half, shapes, old, after=()):
        blocks = [(layer, f, o, 0, half) for f in (False, True) for o in (False, True)]
        return put([new, over_core(new), far, over_core(far)], blocks, shapes, old, after)

    none = lambda at: 0
    cols_a, cols_b = (lambda at: 1 - at[0]), (lambda at: at[0])
    gu = [(wg, mg, vg), (wu, mu, vu)]
    r = ff // 4

    dgu_a, dgu_b, part_gua, far_gua, n_d1, m_d1, v_d1 = middle()
    all_d1 = over_x(n_d1)
    s, part_gub = wide(3, a1t, dgu_b, [n_d1])
    far_gub = over_x(s)
    n_gub, old_gu = update(part_gub, far_gua, 1, gu, cols_b, [])
    all_gub = over_x(n_gub)

    wide_tile = 512
    by_rows = lambda n: spec((wide_tile, n), rows)
    d_out = call(
        back_body, at, (dgu_a, dgu_b, wg, wu, h1, dy),
        [by_rows(ff), by_rows(ff), ANY, ANY, by_rows(d), spec((1, wide_tile, d), lambda i, at: (0, i, 0))],
        shape(tokens, d), by_rows(d), (tokens // wide_tile,), [pltpu.VMEM((2, d, ff), BF16), pltpu.SemaphoreType.DMA((2, 2))], flops=2 * mm, moved=35e6, after=[n_gub],
    )

    def bottom(identity, first, steps, after):
        n, r = 256, d // 4
        cols = 2 * n * steps
        full = spec((r, cols), CORNER, True)
        to_cols = spec((tokens, n), lambda i: (0, first + i))
        return call_with_partner(
            functools.partial(bottom_body, steps), identity, (d_out, a0t, wd, p0, q0),
            [spec((tokens, d), CORNER, True), spec((d, tokens), CORNER, True),
             spec((None, n, d), lambda i: (0, first + i, 0)), to_cols, to_cols],
            [shape(r, cols), shape(r, cols, t=F32)], [full, full], (steps,),
            [pltpu.VMEM((tokens, 2 * n), BF16)] + buffers(steps, 2 * r, 2 * r, 2 * n),
            3 * mm * steps // 9, 50e6 * steps / 9, after,
        )

    n_gua, old_gu = update(part_gua, far_gub, 1, gu, cols_a, old_gu, [d_out])
    all_gua = over_x(n_gua)
    full = spec((r, d), CORNER, True)
    s, part_d0 = call_with_partner(
        down_body, 4, (act0, d_out), [spec((tokens, half), lambda i: (0, i)), spec((tokens, d), CORNER, True)],
        [shape(r, d), shape(r, d, t=F32)], [full, full], (2,), [pltpu.VMEM((2, 2, r + r % 128, d), BF16), pltpu.VMEM((2, r, d), BF16)] + [pltpu.SemaphoreType.DMA((2,))] * 2, mm, 17e6, [n_gua],
    )
    far_d0 = over_x(s)
    s, part_0 = bottom(5, 0, 5, [s])
    far_0 = over_x(s)
    s, part_1 = bottom(6, 5, 4, [s])
    far_1 = over_x(s)
    n_d0, new_d = update(part_d0, far_d0, 0, [(wd, md, vd)], none, [], [s])
    all_d0 = over_x(n_d0)
    both = [wg.shape, wu.shape]
    out_d = put_all(n_d1, all_d1, 1, None, [wd.shape], [], [n_d0])
    out_gu = put_all(n_gub, all_gub, 1, True, both, [], out_d)
    n_0, old_gu = update(part_0, far_0, 0, gu, none, old_gu, out_gu[:1])
    all_0 = over_x(n_0)
    out_gu = put_all(n_gua, all_gua, 1, False, both, out_gu, [n_0])
    third = part_0.shape[1] // 2
    n_top, old_gu = update(part_1, far_1, 0, gu, third, old_gu, out_gu[:1], 7, (0, 5))
    far_top = over_x(n_top)
    n_low, (mg, vg, mu, vu) = update(part_1, far_1, 0, gu, third, old_gu, [n_top], 7, (5, 2))
    far_low = over_x(n_low)
    new_d = pl.pallas_call(
        fill_body,
        in_specs=[ANY] * 5,
        out_specs=[ANY] * 2,
        out_shape=[shape(*md.shape, t=F32)] * 2,
        scratch_shapes=[pltpu.VMEM((2, *m_d1.shape), F32), pltpu.SemaphoreType.DMA((2, 2))],
        input_output_aliases={2: 0, 3: 1},
        compiler_params=pltpu.CompilerParams(vmem_limit_bytes=60 * MIB),
        cost_estimate=pl.CostEstimate(flops=1000000, bytes_accessed=8000000, transcendentals=0),
        name="fill_d",
    )(m_d1, v_d1, *new_d, n_low)
    out_d = put_all(n_d0, all_d0, 0, None, [wd.shape], out_d, [n_low])
    first = n_top.shape[0]
    start = part_0.shape[1] // 2
    blocks = [(0, f, o, low, start) for f in (False, True) for low in (0, first) for o in (False, True)]
    out_gu = put([n_top, over_core(n_top)], blocks[:2], both, out_gu, out_d)
    out_gu = put([n_low, over_core(n_low)], blocks[2:4], both, out_gu)
    out_gu = put_all(n_0, all_0, 0, 0, both, out_gu)
    out_gu = put([far_top, over_core(far_top)], blocks[4:6], both, out_gu)
    out_gu = put([far_low, over_core(far_low)], blocks[6:], both, out_gu)
    return out_gu[0], out_gu[1], out_d[0], mg, mu, new_d[0], vg, vu, new_d[1]


def solution(mesh):
    whole, part = P(None, None, None), P(None, "dp", None)
    seqs = P(("rep", "dp"), None, None)

    return jax.shard_map(
        per_device,
        mesh=mesh,
        in_specs=(seqs, seqs, whole, whole, whole) + (part,) * 6,
        out_specs=(P("rep", None, None),) * 3 + (P("rep", "dp", None),) * 6,
        check_vma=False,
    )
```
